256 devices in a mesh: prow: 16 (over y, x_lo, core), pcol: 16 (over x_hi, z).
Axes of the slice: x: 4 (x_hi: 2, x_lo: 2; x = x_hi * 2 + x_lo), y: 4, z: 8, core: 2. Of those that a mesh axis runs over, the one named last changes fastest.
Arguments:
- ancestor_inverse: float32 [16, 16, 512, 512], P('prow', 'pcol'), may hold values from -0.0625 to 0.0625
- factor_panel: float32 [512, 16, 3, 512], P('pcol', 'prow'), may hold values from -0.75 to 0.75
- pivot_inverse: float32 [3, 512, 512], P(None, 'prow', 'pcol'), may hold values from -6 to 6
- structure: int32 [16, 3], replicated, may hold values from 0 to 1, as said below
Outputs:
- inverse_panel: float32 [512, 16, 3, 512], P('pcol', 'prow')
- diagonal_block: float32 [3, 512, 512], P(None, 'prow', 'pcol')
The draws below stay inside these ranges and needn't reach their ends.
Inputs may be any that keep to these rules, and one draw needn't show every extreme that they name: structure[J, K] is 1 where ancestor J lies in supernode K's structure and 0 elsewhere; the last ancestor, 15, lies in every supernode's structure.
All inputs are finite; a program needn't handle non-finite values.
Results may differ from the reference program's by a relative error of at most 0.00007.
Values sent between devices are 32-bit elements; how exact they have to be, the bound alone decides.
A program may use at most 64 MiB of HBM per device.

```python
import jax
import jax.numpy as jnp
from jax import lax

B = 512
SUPER = 3
M = 16


def draw_structure(key, part):
    drawn_levels = jax.random.randint(key, (M, SUPER), 0, M)
    ancestor_index = jnp.arange(M, dtype=jnp.int32)[:, None]
    return jnp.where(drawn_levels <= ancestor_index, 1, 0).astype(jnp.int32)


def level_of(rng, extent, shards, smallest, largest):
    level = 1.0
    for position, shards_of in shards:
        draws = jax.random.uniform(jax.random.fold_in(jax.random.fold_in(rng, 6), position), (shards_of,), jnp.float32, smallest / len(shards), largest / len(shards))
        level = level * jnp.repeat(jnp.exp(draws), extent[position] // shards_of).reshape((-1,) + (1,) * (len(extent) - 1 - position))
    return level


def gaussian(rng, shape, scale, limit, pieces=(), held_as=jnp.bfloat16):
    factor_of = level_of(rng, shape, pieces, -0.22, 0.18) if pieces else 1.0
    values = jax.random.normal(rng, shape, jnp.float32) * scale * factor_of
    return jnp.minimum(jnp.maximum(values, -limit), limit).astype(held_as)


def setup_inputs(seed: int = 0) -> dict:
    keys = jax.random.split(jax.random.key(seed), 5)
    return {
        "ancestor_inverse": gaussian(keys[0], (M, M, B, B), (M * B) ** -0.5, 0.0625, ((0, 16), (1, 16)), jnp.float32),
        "factor_panel": gaussian(keys[1], (B, M, SUPER, B), 0.125, 0.75, ((0, 16), (1, 16)), jnp.float32),
        "pivot_inverse": gaussian(keys[2], (SUPER, B, B), 1.0, 6.0, ((1, 16), (2, 16)), jnp.float32),
        "structure": draw_structure(jax.random.fold_in(keys[4], 71), 0),
    }


def reference(ancestor_inverse, factor_panel, pivot_inverse, structure):
    struct_float = structure.astype(jnp.float32)
    masked = factor_panel * struct_float[None, :, :, None]

    def one_row(inverse_row):
        return jnp.einsum("Jrt,tJKc->rKc", inverse_row, masked, precision=lax.Precision.HIGHEST, preferred_element_type=jnp.float32)

    product = lax.map(one_row, ancestor_inverse)
    product = jnp.transpose(product, (1, 0, 2, 3))
    inverse_panel = -struct_float[None, :, :, None] * product
    diagonal_block = pivot_inverse - jnp.einsum("riKa,riKb->Kab", masked, inverse_panel, precision=lax.Precision.HIGHEST, preferred_element_type=jnp.float32)
    return inverse_panel, diagonal_block
```

```python
import jax
import jax.numpy as jnp
from jax import lax
from jax.experimental import pallas as pl
from jax.experimental.pallas import tpu as pltpu
from jax.sharding import PartitionSpec as P

F32 = jnp.float32
BF16 = jnp.bfloat16
MESH = pl.DeviceIdType.MESH
ROWS = 32
NSUP = 3
WIDTH = 512
GRID = 16


def split(x):
    high = x.astype(BF16)
    return high, (x - high.astype(F32)).astype(BF16)


def dot(a, b):
    return jnp.dot(a, b, preferred_element_type=F32)


def landing(block, chunk):
    shift = (block - chunk) & 7
    flip = ((block >> 3) ^ (chunk >> 3)) & 1
    turn = jnp.minimum(shift, 8 - shift) & 3
    core = (shift >= 4).astype(jnp.int32)
    return 4 * (((block >> 2) + turn) & 3) + 2 * (((block >> 1) & 1) ^ flip) + core


def chunk_at(row, block):
    turn = ((row >> 2) - (block >> 2)) & 3
    flip = ((row >> 1) & 1) ^ ((block >> 1) & 1)
    back = jnp.where(turn == 0, 4, 8 - turn)
    shift = jnp.where((row & 1) == 1, back, turn)
    return 8 * ((block >> 3) ^ flip) + (((block & 7) - shift) & 7)


def pack(y, put):
    lane = lax.broadcasted_iota(jnp.int32, (8, 128), 1) >> 5
    for g in range(4):
        tiles = [y[8 * u : 8 * u + 8, 128 * g : 128 * g + 128] for u in range(4)]
        for h in range(4):
            out = None
            for u in range(4):
                by = (32 * (u - h)) % 128
                moved = pltpu.roll(tiles[u], by, 1) if by else tiles[u]
                out = moved if out is None else jnp.where(lane == u, moved, out)
            put(4 * g + h, out)


def kernel(
    a_hbm, l_hbm, piv_ref, s_ref,
    y_hbm, d_ref,
    a_in, l_in, a_high, a_low, src, xbuf, pbuf, rbuf, sbuf, xrec, y_out,
    e1s, e1r, e2s, e2r,
    load_sem, ag_send, ag_recv, rs_send, rs_recv, xs_send, xs_recv,
    e1_send, e1_recv, e2_send, e2_recv,
):
    p = lax.axis_index("prow")
    q = lax.axis_index("pcol")
    z = q & 7
    far = q >> 3
    on_diagonal = p == q

    load_l = pltpu.make_async_copy(l_hbm, l_in, load_sem.at[0])
    load_l.start()
    load_a = pltpu.make_async_copy(a_hbm, a_in, load_sem.at[1])
    load_a.start()

    other = p ^ 1
    beside = p ^ 2
    above = (p + 4) & 15
    below = (p - 4) & 15
    z_up = (q & 8) + ((z + 1) & 7)
    z_down = (q & 8) + ((z - 1) & 7)
    across = q ^ 8

    barrier = pltpu.get_barrier_semaphore()
    for device in ((other, q), (beside, q), (above, q), (below, q), (p, z_up), (p, z_down), (p, across)):
        pl.semaphore_signal(barrier, inc=1, device_id=device, device_id_type=MESH)

    def greet(t, carry):
        @pl.when(jnp.logical_or(t != p, p != q))
        def _():
            pl.semaphore_signal(barrier, inc=1, device_id=(t, p), device_id_type=MESH)

        @pl.when(jnp.logical_or(t != q, p != q))
        def _():
            pl.semaphore_signal(barrier, inc=1, device_id=(q, t), device_id_type=MESH)

        return carry

    lax.fori_loop(0, GRID, greet, 0)

    load_l.wait()
    for k in range(NSUP):
        for g in range(4):
            src[k, :, 128 * g : 128 * g + 128] = l_in[pl.ds(4 * k + g, ROWS, stride=12), :]
    load_a.wait()
    a_high[...], a_low[...] = split(a_in[...])
    pl.semaphore_wait(barrier, jnp.where(on_diagonal, 37, 39))

    def remote(source, target, send, recv, device):
        return pltpu.make_async_remote_copy(
            src_ref=source, dst_ref=target, send_sem=send, recv_sem=recv, device_id=device, device_id_type=MESH
        )

    def rows_of(row):
        return pl.ds(pl.multiple_of(ROWS * chunk_at(row, q), ROWS), ROWS)

    kinds = (p, p ^ 2, below, below ^ 2, above, above ^ 2, (p + 8) & 15, ((p + 8) & 15) ^ 2)
    kinds = kinds + tuple(kind ^ 1 for kind in kinds)
    where = [rows_of(kind) for kind in kinds]

    def piece(k, kind):
        return xbuf.at[k, where[kind], :]

    sends = []

    def send_piece(k, kind, slot, as_kind, device):
        copy = remote(piece(k, kind), piece(k, kind), ag_send.at[k, slot], ag_recv.at[k, as_kind], (device, q))
        copy.start()
        sends.append(copy)

    def wait_piece(k, kind):
        remote(piece(k, kind), piece(k, kind), ag_send.at[k, 0], ag_recv.at[k, kind], (other, q)).wait_recv()

    first = landing(p, q)
    first_rows = pl.ds(pl.multiple_of(ROWS * q, ROWS), ROWS)
    stays = jnp.logical_and(first == p, on_diagonal)

    def first_copy(k):
        return remote(src.at[k], xbuf.at[k, first_rows, :], ag_send.at[k, 0], ag_recv.at[k, 0], (first, p))

    def st_first(k):
        @pl.when(jnp.logical_not(stays))
        def _():
            first_copy(k).start()

        @pl.when(stays)
        def _():
            xbuf[k, first_rows, :] = src[k]

    mine = jnp.logical_and(landing(q, q) == p, on_diagonal)

    def st_own(k):
        @pl.when(jnp.logical_not(mine))
        def _():
            wait_piece(k, 0)

        send_piece(k, 0, 1, 1, beside)
        send_piece(k, 0, 2, 2, above)
        send_piece(k, 0, 3, 4, below)
        send_piece(k, 0, 8, 8, other)

    def st_beside(k):
        wait_piece(k, 1)
        send_piece(k, 1, 4, 3, above)
        send_piece(k, 1, 5, 5, below)
        send_piece(k, 1, 9, 9, other)

    def st_ring(k):
        wait_piece(k, 2)
        send_piece(k, 2, 6, 6, above)
        send_piece(k, 2, 10, 10, other)
        wait_piece(k, 4)
        send_piece(k, 4, 12, 12, other)
        wait_piece(k, 5)
        send_piece(k, 5, 7, 7, below)
        send_piece(k, 5, 13, 13, other)
        wait_piece(k, 3)
        send_piece(k, 3, 11, 11, other)

    def st_last(k):
        wait_piece(k, 6)
        send_piece(k, 6, 14, 14, other)
        wait_piece(k, 7)
        send_piece(k, 7, 15, 15, other)

    down_steps = (4, 3)
    up_steps = (3, 4)
    steps = [[down_steps[h], up_steps[h]] for h in range(2)]

    def block_rows(h, d):
        return pl.ds(pl.multiple_of(256 * h + ROWS * d, ROWS), ROWS)

    def sent_block(h, way, t):
        left = steps[h][way] - t
        return (z - left) & 7 if way == 0 else (z + left) & 7

    def send_sum(k, h, way, t):
        copy = remote(
            pbuf.at[k, block_rows(h, sent_block(h, way, t)), :],
            rbuf.at[k, h, way, t],
            rs_send.at[k, h, way, t],
            rs_recv.at[k, h, way, t],
            (p, z_down if way == 0 else z_up),
        )
        copy.start()
        sends.append(copy)

    def wait_sum(k, h, way, t):
        remote(
            rbuf.at[k, h, way, t], rbuf.at[k, h, way, t], rs_send.at[k, h, way, t], rs_recv.at[k, h, way, t], (p, z_up)
        ).wait_recv()

    def mask_of(k, index):
        return s_ref[k, index].astype(F32)

    def st_product(k):
        for kind in range(8, 16):
            wait_piece(k, kind)
        mask = mask_of(k, q)
        x_high, x_low = split(xbuf[k] * mask)
        for m in range(4):
            at = slice(128 * m, 128 * m + 128)
            pbuf[k, at, :] = dot(a_high[at, :], x_high) + dot(a_high[at, :], x_low) + dot(a_low[at, :], x_high)
        for h in range(2):
            for way in range(2):
                send_sum(k, h, way, 0)

    def st_sum(k, t):
        for h in range(2):
            for way in range(2):
                last = steps[h][way] - 1
                if t > last:
                    continue
                wait_sum(k, h, way, t)
                if t < last:
                    rows = block_rows(h, sent_block(h, way, t + 1))
                    pbuf[k, rows, :] = pbuf[k, rows, :] + rbuf[k, h, way, t]
                    send_sum(k, h, way, t + 1)
        if t == 3:
            for h in range(2):
                total = pbuf[k, block_rows(h, z), :]
                for way in range(2):
                    total = total + rbuf[k, h, way, steps[h][way] - 1]
                sbuf[k, h] = total
            copy = remote(sbuf.at[k, 1 - far], xrec.at[k], xs_send.at[k], xs_recv.at[k], (p, across))
            copy.start()
            sends.append(copy)

    def exchange(k, source, target, send, recv):
        def copy(t):
            return remote(source.at[k, t], target.at[k, q], send.at[k, t], recv.at[k, q], (t, p))

        def one(i, carry):
            copy((p + i) & 15).start()
            return carry

        @pl.when(jnp.logical_not(on_diagonal))
        def _():
            copy(p).start()

        @pl.when(on_diagonal)
        def _():
            target[k, q] = source[k, p]

        lax.fori_loop(1, GRID, one, 0)

    def arrived(k, target, send, recv):
        def one(j, carry):
            @pl.when(jnp.logical_or(j != q, p != q))
            def _():
                remote(target.at[k, j], target.at[k, j], send.at[k, j], recv.at[k, j], (other, q)).wait_recv()

            return carry

        lax.fori_loop(0, GRID, one, 0)

    def left(k, source, send, recv):
        def one(t, carry):
            @pl.when(jnp.logical_or(t != p, p != q))
            def _():
                remote(source.at[k, t], source.at[k, t], send.at[k, t], recv.at[k, t], (other, q)).wait_send()

            return carry

        lax.fori_loop(0, GRID, one, 0)

    def st_panel(k):
        remote(xrec.at[k], xrec.at[k], xs_send.at[k], xs_recv.at[k], (p, across)).wait_recv()
        y = (sbuf[k, far] + xrec[k]) * (-mask_of(k, p))

        def put(t, tile):
            e1s[k, t] = tile

        pack(y, put)
        exchange(k, e1s, e1r, e1_send, e1_recv)
        for g in range(4):
            y_out[pl.ds(4 * k + g, ROWS, stride=12), :] = y[:, 128 * g : 128 * g + 128]

    def st_diagonal(k):
        arrived(k, e1r, e1_send, e1_recv)
        turned = e1r[k].reshape(128, 128).T
        x = xbuf[k].reshape(GRID, 4, 8, WIDTH)
        total = None
        for u in range(4):
            y_high, y_low = split(turned[32 * u : 32 * u + 32, :])
            x_high, x_low = split(x[:, u].reshape(128, WIDTH))
            term = dot(y_high, x_high) + dot(y_high, x_low) + dot(y_low, x_high)
            total = term if total is None else total + term

        def put(t, tile):
            e2s[k, t] = tile

        pack(total, put)
        exchange(k, e2s, e2r, e2_send, e2_recv)

    def st_result(k):
        arrived(k, e2r, e2_send, e2_recv)
        total = jnp.sum(e2r[k], axis=0)
        parts = [total] + [pltpu.roll(total, 128 - 32 * u, 1) for u in range(1, 4)]
        square = jnp.concatenate(parts + [jnp.zeros((96, 128), F32)], axis=0).T
        d_ref[k] = piv_ref[k] - square[:32, :32]

    events = []
    for k in range(NSUP):
        events.append((-10 + k, k, st_first))
        events.append((0 + 3 * k, k, st_own))
        events.append((2.5 + 3 * k, k, st_beside))
        events.append((5 + 4 * k, k, st_ring))
        events.append((8 + 4 * k, k, st_last))
        events.append((10 + 4 * k, k, st_product))
        for t in range(4):
            events.append((14 + 4.5 * t + 6 * k, k, lambda k, t=t: st_sum(k, t)))
        events.append((32 + 6 * k, k, st_panel))
        events.append((40 + 6 * k, k, st_diagonal))
        events.append((48 + 6 * k, k, st_result))
    for _, k, stage in sorted(events, key=lambda e: e[0]):
        stage(k)

    store = pltpu.make_async_copy(y_out, y_hbm, load_sem.at[0])
    store.start()
    for k in range(NSUP):

        @pl.when(jnp.logical_not(stays))
        def _():
            first_copy(k).wait_send()

        left(k, e1s, e1_send, e1_recv)
        left(k, e2s, e2_send, e2_recv)
    for copy in sends:
        copy.wait_send()
    store.wait()


def body(ancestor_inverse, factor_panel, pivot_inverse, structure):
    vmem = pl.BlockSpec(memory_space=pltpu.VMEM)
    hbm = pl.BlockSpec(memory_space=pl.ANY)
    dma = pltpu.SemaphoreType.DMA
    panel, diagonal = pl.pallas_call(
        kernel,
        out_shape=(
            jax.ShapeDtypeStruct((ROWS * NSUP * 4, 128), F32),
            jax.ShapeDtypeStruct(pivot_inverse.shape, F32),
        ),
        in_specs=[hbm, hbm, vmem, pl.BlockSpec(memory_space=pltpu.SMEM)],
        out_specs=(hbm, vmem),
        scratch_shapes=[
            pltpu.VMEM((WIDTH, WIDTH), F32),
            pltpu.VMEM((ROWS * NSUP * 4, 128), F32),
            pltpu.VMEM((WIDTH, WIDTH), BF16),
            pltpu.VMEM((WIDTH, WIDTH), BF16),
            pltpu.VMEM((NSUP, ROWS, WIDTH), F32),
            pltpu.VMEM((NSUP, WIDTH, WIDTH), F32),
            pltpu.VMEM((NSUP, WIDTH, WIDTH), F32),
            pltpu.VMEM((NSUP, 2, 2, 4, ROWS, WIDTH), F32),
            pltpu.VMEM((NSUP, 2, ROWS, WIDTH), F32),
            pltpu.VMEM((NSUP, ROWS, WIDTH), F32),
            pltpu.VMEM((ROWS * NSUP * 4, 128), F32),
            pltpu.VMEM((NSUP, GRID, 8, 128), F32),
            pltpu.VMEM((NSUP, GRID, 8, 128), F32),
            pltpu.VMEM((NSUP, GRID, 8, 128), F32),
            pltpu.VMEM((NSUP, GRID, 8, 128), F32),
            dma((2,)),
            dma((NSUP, 16)),
            dma((NSUP, 16)),
            dma((NSUP, 2, 2, 4)),
            dma((NSUP, 2, 2, 4)),
            dma((NSUP,)),
            dma((NSUP,)),
            dma((NSUP, GRID)),
            dma((NSUP, GRID)),
            dma((NSUP, GRID)),
            dma((NSUP, GRID)),
        ],
        compiler_params=pltpu.CompilerParams(
            collective_id=0, has_side_effects=True, vmem_limit_bytes=48 * 1024 * 1024
        ),
        name="level",
    )(
        ancestor_inverse.reshape(WIDTH, WIDTH),
        factor_panel.reshape(ROWS * NSUP * 4, 128),
        pivot_inverse,
        structure.T,
    )
    return panel.reshape(ROWS, 1, NSUP, WIDTH), diagonal


def solution(mesh):
    return jax.shard_map(
        body,
        mesh=mesh,
        in_specs=(
            P("prow", "pcol", None, None),
            P("pcol", "prow", None, None),
            P(None, "prow", "pcol"),
            P(),
        ),
        out_specs=(P("pcol", "prow", None, None), P(None, "prow", "pcol")),
        check_vma=False,
    )
```

```python
import jax
import jax.numpy as jnp
from jax import lax
from jax.experimental import pallas as pl
from jax.experimental.pallas import tpu as pltpu
from jax.sharding import PartitionSpec as P

F32 = jnp.float32
BF16 = jnp.bfloat16
MESH = pl.DeviceIdType.MESH
ROWS = 32
NSUP = 3
WIDTH = 512
GRID = 16


def split(x):
    high = x.astype(BF16)
    return high, (x - high.astype(F32)).astype(BF16)


def dot(a, b):
    return jnp.dot(a, b, preferred_element_type=F32)


def passing(row, chunk):
    bit = chunk & 1
    turn = 2 * (((row >> 1) ^ (chunk >> 1)) & 1) + (((chunk >> 2) & 1) ^ bit)
    return row ^ (4 * turn + bit)


def landing(row, block, chunk):
    return row ^ (2 * (((block >> 3) ^ (chunk >> 3)) & 1))


def chunk_at(row, block):
    high = ((row >> 1) ^ (block >> 1)) & 1
    low = row & 1
    middle = ((row >> 3) ^ (block >> 3)) & 1
    third = ((row >> 2) ^ block ^ low) & 1
    return block ^ (8 * high + 4 * third + 2 * middle + low)


def pack(y, put):
    lane = lax.broadcasted_iota(jnp.int32, (8, 128), 1) >> 5
    for g in range(4):
        tiles = [y[8 * u : 8 * u + 8, 128 * g : 128 * g + 128] for u in range(4)]
        for h in range(4):
            out = None
            for u in range(4):
                by = (32 * (u - h)) % 128
                moved = pltpu.roll(tiles[u], by, 1) if by else tiles[u]
                out = moved if out is None else jnp.where(lane == u, moved, out)
            put(4 * g + h, out)


def kernel(
    a_hbm, l_hbm, piv_hbm, s_hbm,
    y_out, d_ref,
    a_in, l_in, piv_in, s_in, a_high, a_low, src, taken, xbuf, pbuf, rbuf, sbuf, xrec, ybuf,
    e1s, e1r, e2s, e2r,
    load_sem, a_send, a_recv, xg_send, xg_recv, rs_send, rs_recv, xs_send, xs_recv, yg_send, yg_recv,
    e1_send, e1_recv, e2_send, e2_recv,
):
    p = lax.axis_index("prow")
    q = lax.axis_index("pcol")
    z = q & 7
    far = q >> 3

    loads = [
        pltpu.make_async_copy(source, target, load_sem.at[n])
        for n, (source, target) in enumerate(((l_hbm, l_in), (a_hbm, a_in), (s_hbm, s_in), (piv_hbm, piv_in)))
    ]
    for load in loads:
        load.start()

    other = p ^ 1
    beside = p ^ 2
    above = (p + 4) & 15
    below = (p - 4) & 15
    z_up = (q & 8) + ((z + 1) & 7)
    z_down = (q & 8) + ((z - 1) & 7)
    across = q ^ 8

    taker = passing(p, q)
    keeps = taker == p
    block = taker
    target_row = landing(p, block, q)
    stays = block == q
    origin = chunk_at(p, q)
    origin_row = landing(p, q, origin)

    barrier = pltpu.get_barrier_semaphore()
    for device in ((other, q), (beside, q), (above, q), (below, q), (p, z_up), (p, z_down), (p, across)):
        pl.semaphore_signal(barrier, inc=1, device_id=device, device_id_type=MESH)

    @pl.when(jnp.logical_not(keeps))
    def _():
        pl.semaphore_signal(barrier, inc=1, device_id=(taker, q), device_id_type=MESH)

    @pl.when(jnp.logical_not(stays))
    def _():
        pl.semaphore_signal(barrier, inc=1, device_id=(target_row, block), device_id_type=MESH)

    @pl.when(origin != q)
    def _():
        pl.semaphore_signal(barrier, inc=1, device_id=(origin_row, origin), device_id_type=MESH)

    loads[0].wait()
    for k in range(NSUP):
        for g in range(4):
            src[k, :, 128 * g : 128 * g + 128] = l_in[pl.ds(4 * k + g, ROWS, stride=12), :]
    with jax.named_scope("barrier"):
        pl.semaphore_wait(
            barrier, jnp.where(keeps, 7, 8) + jnp.where(stays, 0, 1) + jnp.where(origin == q, 0, 1)
        )

    def remote(source, target, send, recv, device):
        return pltpu.make_async_remote_copy(
            src_ref=source, dst_ref=target, send_sem=send, recv_sem=recv, device_id=device, device_id_type=MESH
        )

    sends = []

    def go(copy):
        copy.start()
        sends.append(copy)

    opposite = (p + 8) & 15
    kinds = (p, beside, below, below ^ 2, above, above ^ 2, opposite, opposite ^ 2)
    kinds = kinds + tuple(kind ^ 1 for kind in kinds)

    class Gather:
        def __init__(self, buffer, slots, send, recv):
            self.buffer, self.send, self.recv = buffer, send, recv
            self.where = [pl.ds(pl.multiple_of(ROWS * slot, ROWS), ROWS) for slot in slots]

        def piece(self, k, kind):
            return self.buffer.at[k, self.where[kind], :]

        def push(self, k, kind, slot, as_kind, row):
            piece = self.piece(k, kind)
            go(remote(piece, piece, self.send.at[k, slot], self.recv.at[k, as_kind], (row, q)))

        def wait(self, k, kind):
            piece = self.piece(k, kind)
            remote(piece, piece, self.send.at[k, 0], self.recv.at[k, kind], (other, q)).wait_recv()

        def own(self, k):
            self.push(k, 0, 1, 1, beside)
            self.push(k, 0, 2, 2, above)
            self.push(k, 0, 3, 4, below)
            self.push(k, 0, 8, 8, other)

        def second(self, k):
            self.wait(k, 1)
            self.push(k, 1, 4, 3, above)
            self.push(k, 1, 5, 5, below)
            self.push(k, 1, 9, 9, other)

        def ring(self, k):
            self.wait(k, 2)
            self.push(k, 2, 6, 6, above)
            self.push(k, 2, 10, 10, other)
            self.wait(k, 4)
            self.push(k, 4, 12, 12, other)
            self.wait(k, 5)
            self.push(k, 5, 7, 7, below)
            self.push(k, 5, 13, 13, other)
            self.wait(k, 3)
            self.push(k, 3, 11, 11, other)

        def last(self, k):
            self.wait(k, 6)
            self.push(k, 6, 14, 14, other)
            self.wait(k, 7)
            self.push(k, 7, 15, 15, other)

        def rest(self, k):
            for kind in range(8, 16):
                self.wait(k, kind)

    gx = Gather(xbuf, [chunk_at(kind, q) for kind in kinds], xg_send, xg_recv)
    gy = Gather(ybuf, list(kinds), yg_send, yg_recv)

    def take_copy(k):
        return remote(src.at[k], taken.at[k], a_send.at[k], a_recv.at[k], (taker, q))

    def land_copy(k):
        rows = pl.ds(pl.multiple_of(ROWS * q, ROWS), ROWS)
        return remote(taken.at[k], xbuf.at[k, rows, :], xg_send.at[k, 0], xg_recv.at[k, 0], (target_row, block))

    for k in range(NSUP):

        @pl.when(jnp.logical_not(keeps))
        def _():
            take_copy(k).start()

        @pl.when(keeps)
        def _():
            taken[k] = src[k]

    def st_take(k):
        @pl.when(jnp.logical_not(keeps))
        def _():
            take_copy(k).wait_recv()

        @pl.when(jnp.logical_not(stays))
        def _():
            land_copy(k).start()

        @pl.when(stays)
        def _():
            xbuf[k, gx.where[0], :] = taken[k]

    def st_prepare(k):
        loads[1].wait()
        a_high[...], a_low[...] = split(a_in[...])
        for n in range(NSUP):

            def put(t, tile, n=n):
                e1s[t, 8 * n : 8 * n + 8, :] = tile

            pack(src[n], put)
        loads[2].wait()
        loads[3].wait()

    def st_own(k):
        @pl.when(origin != q)
        def _():
            gx.wait(k, 0)

        gx.own(k)

    down_steps = (4, 3)
    up_steps = (3, 4)
    steps = [[down_steps[h], up_steps[h]] for h in range(2)]

    def block_rows(h, d):
        return pl.ds(pl.multiple_of(256 * h + ROWS * d, ROWS), ROWS)

    def sent_block(h, way, t):
        left = steps[h][way] - t
        return (z - left) & 7 if way == 0 else (z + left) & 7

    def send_sum(k, h, way, t):
        go(
            remote(
                pbuf.at[k, block_rows(h, sent_block(h, way, t)), :],
                rbuf.at[k, h, way, t],
                rs_send.at[k, h, way, t],
                rs_recv.at[k, h, way, t],
                (p, z_down if way == 0 else z_up),
            )
        )

    def wait_sum(k, h, way, t):
        remote(
            rbuf.at[k, h, way, t], rbuf.at[k, h, way, t], rs_send.at[k, h, way, t], rs_recv.at[k, h, way, t], (p, z_up)
        ).wait_recv()

    def mask_of(k, index):
        return s_in[k, index].astype(F32)

    def st_product(k):
        gx.rest(k)
        x_high, x_low = split(xbuf[k] * mask_of(k, q))
        for m in range(4):
            at = slice(128 * m, 128 * m + 128)
            pbuf[k, at, :] = dot(a_high[at, :], x_high) + dot(a_high[at, :], x_low) + dot(a_low[at, :], x_high)
        for h in range(2):
            for way in range(2):
                send_sum(k, h, way, 0)

    def st_sum(k, t):
        for h in range(2):
            for way in range(2):
                last = steps[h][way] - 1
                if t > last:
                    continue
                wait_sum(k, h, way, t)
                if t < last:
                    rows = block_rows(h, sent_block(h, way, t + 1))
                    pbuf[k, rows, :] = pbuf[k, rows, :] + rbuf[k, h, way, t]
                    send_sum(k, h, way, t + 1)
        if t == 3:
            for h in range(2):
                total = pbuf[k, block_rows(h, z), :]
                for way in range(2):
                    total = total + rbuf[k, h, way, steps[h][way] - 1]
                sbuf[k, h] = total
            go(remote(sbuf.at[k, 1 - far], xrec.at[k], xs_send.at[k], xs_recv.at[k], (p, across)))

    def st_spread(k):
        def one(i, carry):
            t = (p + i) & 15
            remote(e1s.at[t], e1r.at[p], e1_send.at[t], e1_recv.at[p], (t, q)).start()
            return carry

        lax.fori_loop(1, GRID, one, 0)
        e1r[p] = e1s[p]

    def st_panel(k):
        remote(xrec.at[k], xrec.at[k], xs_send.at[k], xs_recv.at[k], (p, across)).wait_recv()
        y = (sbuf[k, far] + xrec[k]) * (-mask_of(k, p))
        ybuf[k, gy.where[0], :] = y
        for g in range(4):
            y_out[pl.ds(4 * k + g, ROWS, stride=12), :] = y[:, 128 * g : 128 * g + 128]
        gy.own(k)

    def st_spread_wait(k):
        def one(i, carry):
            t = (p + i) & 15
            remote(e1r.at[t], e1r.at[t], e1_send.at[t], e1_recv.at[t], (other, q)).wait_recv()
            return carry

        lax.fori_loop(1, GRID, one, 0)

    def st_diagonal(k):
        turned = e1r[:, 8 * k : 8 * k + 8, :].reshape(128, 128).T
        left = [split(turned[32 * u : 32 * u + 32, :]) for u in range(4)]
        gy.rest(k)
        y = ybuf[k].reshape(GRID, 4, 8, WIDTH)
        total = None
        for u in range(4):
            l_high, l_low = left[u]
            y_high, y_low = split(y[:, u].reshape(128, WIDTH))
            term = dot(l_high, y_high) + dot(l_high, y_low) + dot(l_low, y_high)
            total = term if total is None else total + term

        def put(t, tile):
            e2s[k, t] = tile

        pack(total, put)

        def one(i, carry):
            t = (q + i) & 15
            remote(e2s.at[k, t], e2r.at[k, q], e2_send.at[k, t], e2_recv.at[k, q], (p, t)).start()
            return carry

        lax.fori_loop(1, GRID, one, 0)
        e2r[k, q] = e2s[k, q]

    def st_result(k):
        def one(i, carry):
            t = (q + i) & 15
            remote(e2r.at[k, t], e2r.at[k, t], e2_send.at[k, t], e2_recv.at[k, t], (other, q)).wait_recv()
            return carry

        lax.fori_loop(1, GRID, one, 0)
        total = jnp.sum(e2r[k], axis=0)
        parts = [total] + [pltpu.roll(total, 128 - 32 * u, 1) for u in range(1, 4)]
        square = jnp.concatenate(parts, axis=0)
        d_ref[k] = piv_in[k] - square[:, :ROWS]

    events = [(-8, 0, "prepare", st_prepare)]
    for k in range(NSUP):
        events.append((-9 + k, k, "take", st_take))
        events.append((0 + 3 * k, k, "own", st_own))
        events.append((2.5 + 3 * k, k, "second", gx.second))
        events.append((5 + 4 * k, k, "ring", gx.ring))
        events.append((8 + 4 * k, k, "last", gx.last))
        events.append((10 + 4 * k, k, "product", st_product))
        for t in range(4):
            events.append((14 + 5 * (t + k) - 0.1 * k, k, f"sum{t}", lambda k, t=t: st_sum(k, t)))
        events.append((35 + 5 * k, k, "panel", st_panel))
        events.append((38 + 5 * k, k, "ysecond", gy.second))
        events.append((41 + 5 * k, k, "yring", gy.ring))
        events.append((44 + 5 * k, k, "ylast", gy.last))
        events.append((46 + 5 * k, k, "diagonal", st_diagonal))
        events.append((54 + 5 * k, k, "result", st_result))
    events.append((18.5, 0, "spread", st_spread))
    events.append((43.5, 0, "arrived", st_spread_wait))
    for _, k, name, stage in sorted(events, key=lambda e: e[0]):
        with jax.named_scope(f"{name}_{k}"):
            stage(k)

    for k in range(NSUP):

        @pl.when(jnp.logical_not(keeps))
        def _():
            take_copy(k).wait_send()

        @pl.when(jnp.logical_not(stays))
        def _():
            land_copy(k).wait_send()

        def one(i, carry, k=k):
            t = (q + i) & 15
            remote(e2s.at[k, t], e2s.at[k, t], e2_send.at[k, t], e2_recv.at[k, t], (other, q)).wait_send()
            return carry

        lax.fori_loop(1, GRID, one, 0)

    def one(i, carry):
        t = (p + i) & 15
        remote(e1s.at[t], e1s.at[t], e1_send.at[t], e1_recv.at[t], (other, q)).wait_send()
        return carry

    lax.fori_loop(1, GRID, one, 0)
    for copy in sends:
        copy.wait_send()


def body(ancestor_inverse, factor_panel, pivot_inverse, structure):
    vmem = pl.BlockSpec(memory_space=pltpu.VMEM)
    hbm = pl.BlockSpec(memory_space=pltpu.HBM)
    dma = pltpu.SemaphoreType.DMA
    panel, diagonal = pl.pallas_call(
        kernel,
        out_shape=(
            jax.ShapeDtypeStruct((ROWS * NSUP * 4, 128), F32),
            jax.ShapeDtypeStruct(pivot_inverse.shape, F32),
        ),
        in_specs=[hbm] * 4,
        out_specs=(vmem, vmem),
        scratch_shapes=[
            pltpu.VMEM((WIDTH, WIDTH), F32),
            pltpu.VMEM((ROWS * NSUP * 4, 128), F32),
            pltpu.VMEM((NSUP, ROWS, ROWS), F32),
            pltpu.SMEM((NSUP, GRID), jnp.int32),
            pltpu.VMEM((WIDTH, WIDTH), BF16),
            pltpu.VMEM((WIDTH, WIDTH), BF16),
            pltpu.VMEM((NSUP, ROWS, WIDTH), F32),
            pltpu.VMEM((NSUP, ROWS, WIDTH), F32),
            pltpu.VMEM((NSUP, WIDTH, WIDTH), F32),
            pltpu.VMEM((NSUP, WIDTH, WIDTH), F32),
            pltpu.VMEM((NSUP, 2, 2, 4, ROWS, WIDTH), F32),
            pltpu.VMEM((NSUP, 2, ROWS, WIDTH), F32),
            pltpu.VMEM((NSUP, ROWS, WIDTH), F32),
            pltpu.VMEM((NSUP, WIDTH, WIDTH), F32),
            pltpu.VMEM((GRID, NSUP * 8, 128), F32),
            pltpu.VMEM((GRID, NSUP * 8, 128), F32),
            pltpu.VMEM((NSUP, GRID, 8, 128), F32),
            pltpu.VMEM((NSUP, GRID, 8, 128), F32),
            dma((4,)),
            dma((NSUP,)),
            dma((NSUP,)),
            dma((NSUP, 16)),
            dma((NSUP, 16)),
            dma((NSUP, 2, 2, 4)),
            dma((NSUP, 2, 2, 4)),
            dma((NSUP,)),
            dma((NSUP,)),
            dma((NSUP, 16)),
            dma((NSUP, 16)),
            dma((GRID,)),
            dma((GRID,)),
            dma((NSUP, GRID)),
            dma((NSUP, GRID)),
        ],
        compiler_params=pltpu.CompilerParams(
            collective_id=0, has_side_effects=True, vmem_limit_bytes=40 * 1024 * 1024
        ),
        name="level",
    )(
        ancestor_inverse.reshape(WIDTH, WIDTH),
        factor_panel.reshape(ROWS * NSUP * 4, 128),
        pivot_inverse,
        structure.T,
    )
    return panel.reshape(ROWS, 1, NSUP, WIDTH), diagonal


def solution(mesh):
    return jax.shard_map(
        body,
        mesh=mesh,
        in_specs=(
            P("prow", "pcol", None, None),
            P("pcol", "prow", None, None),
            P(None, "prow", "pcol"),
            P(),
        ),
        out_specs=(P("pcol", "prow", None, None), P(None, "prow", "pcol")),
        check_vma=False,
    )
```

```python
import jax
import jax.numpy as jnp
from jax import lax
from jax.experimental import pallas as pl
from jax.experimental.pallas import tpu as pltpu
from jax.sharding import PartitionSpec as P

F32 = jnp.float32
BF16 = jnp.bfloat16
MESH = pl.DeviceIdType.MESH
ROWS = 32
NSUP = 3
WIDTH = 512
GRID = 16
UNITS = 6
COLS = 256
IN_FLIGHT = 3
FIRST_ACROSS = (1, 3)


VMEM_LIMIT = 40 * 1024 * 1024


def plan():
    when = {("prepare", 0): -8.0}
    product = []
    for k in range(UNITS):
        when["take", k] = -9 + 0.1 * k
        when["own", k] = 1.6 * k
        when["second", k] = 1.6 * k + 0.8
        when["forward", k] = 4.5 + 2.9 * k
        when["product", k] = 6.5 + 2.9 * k
        product.append(7.2 + 2.9 * k)
    when["spread", 0] = product[-1] + 0.1
    ready, x_free = {}, 0.0
    for k in range(UNITS):
        ready[k] = product[k]
        if k in FIRST_ACROSS:
            x_free = max(x_free, product[k]) + 5.4
            ready[k] = x_free + 2.5
    waiting = sorted(range(UNITS), key=lambda k: ready[k])
    flying, free, ended = [], 0.0, {}
    while waiting or flying:
        while waiting and len(flying) < IN_FLIGHT:
            k = waiting.pop(0)
            start = max(ready[k], max(ended.values(), default=0.0) if len(ended) + len(flying) >= IN_FLIGHT else 0.0)
            when["launch", k] = start
            flying.append((start, k, 0))
        start, k, t = min(flying)
        flying.remove((start, k, t))
        free = max(free, start) + (0.7 if k in FIRST_ACROSS else 1.4)
        when[f"sum{t}", k] = free + 1.9
        if t < 3:
            flying.append((free + 1.9, k, t + 1))
        else:
            ended[k] = free + 1.9
    free, here = 0.0, {}
    for k in sorted(range(UNITS), key=lambda k: ended[k]):
        when["panel", k] = ended[k] + (0.1 if k in FIRST_ACROSS else 3.5)
        free = max(free, when["panel", k]) + 2.9
        here[k] = free + 3.5
    for n in range(NSUP):
        when["diagonal", n] = max(here[2 * n], here[2 * n + 1])
        when["result", n] = when["diagonal", n] + 7.5
    when["arrived", 0] = min(when["diagonal", n] for n in range(NSUP)) - 0.1
    return [event for event, _ in sorted(when.items(), key=lambda item: item[1])]


ORDER = plan()


def split(x):
    high = x.astype(BF16)
    return high, (x - high.astype(F32)).astype(BF16)


def dot(a, b):
    return jnp.dot(a, b, preferred_element_type=F32)


def passing(row, chunk):
    bit = chunk & 1
    turn = 2 * (((row >> 1) ^ (chunk >> 1)) & 1) + (((chunk >> 2) & 1) ^ bit)
    return row ^ (4 * turn + bit)


def landing(row, block, chunk):
    return row ^ (2 * (((block >> 3) ^ (chunk >> 3)) & 1))


def chunk_at(row, block):
    high = ((row >> 1) ^ (block >> 1)) & 1
    low = row & 1
    middle = ((row >> 3) ^ (block >> 3)) & 1
    third = ((row >> 2) ^ block ^ low) & 1
    return block ^ (8 * high + 4 * third + 2 * middle + low)


def pack(y, put):
    lane = lax.broadcasted_iota(jnp.int32, (8, 128), 1) >> 5
    for g in range(y.shape[1] // 128):
        tiles = [y[8 * u : 8 * u + 8, 128 * g : 128 * g + 128] for u in range(4)]
        for h in range(4):
            out = None
            for u in range(4):
                by = (32 * (u - h)) % 128
                moved = pltpu.roll(tiles[u], by, 1) if by else tiles[u]
                out = moved if out is None else jnp.where(lane == u, moved, out)
            put(4 * g + h, out)


def kernel(
    a_hbm, l_hbm, piv_hbm, s_hbm,
    y_out, d_out,
    a_in, l_in, piv_in, s_in, a_high, a_low, src, taken, xbuf, pbuf, rbuf, sbuf, xrec, xhalf, ybuf,
    e1s, e1r, e2s, e2r,
    load_sem, a_send, a_recv, xg_send, xg_recv, rs_send, rs_recv, xs_send, xs_recv, yg_send, yg_recv,
    e1_send, e1_recv, e2_send, e2_recv,
):
    p = lax.axis_index("prow")
    q = lax.axis_index("pcol")
    z = q & 7
    far = q >> 3

    loads = [
        pltpu.make_async_copy(source, target, load_sem.at[n])
        for n, (source, target) in enumerate(((l_hbm, l_in), (a_hbm, a_in), (s_hbm, s_in), (piv_hbm, piv_in)))
    ]
    for load in loads:
        load.start()

    other = p ^ 1
    beside = p ^ 2
    above = (p + 4) & 15
    below = (p - 4) & 15
    z_up = (q & 8) + ((z + 1) & 7)
    z_down = (q & 8) + ((z - 1) & 7)
    across = q ^ 8

    taker = passing(p, q)
    keeps = taker == p
    block = taker
    target_row = landing(p, block, q)
    stays = block == q
    origin = chunk_at(p, q)
    origin_row = landing(p, q, origin)
    second = chunk_at(beside, q)
    second_row = landing(beside, q, second)

    barrier = pltpu.get_barrier_semaphore()
    opposite = (p + 8) & 15
    for device in (
        (other, q), (beside, q), (above, q), (below, q), (opposite, q), (p, z_up), (p, z_down), (p, across)
    ):
        pl.semaphore_signal(barrier, inc=1, device_id=device, device_id_type=MESH)

    @pl.when(jnp.logical_not(keeps))
    def _():
        pl.semaphore_signal(barrier, inc=1, device_id=(taker, q), device_id_type=MESH)

    @pl.when(jnp.logical_not(stays))
    def _():
        pl.semaphore_signal(barrier, inc=1, device_id=(target_row, block), device_id_type=MESH)

    @pl.when(origin != q)
    def _():
        pl.semaphore_signal(barrier, inc=1, device_id=(origin_row, origin), device_id_type=MESH)

    pl.semaphore_signal(barrier, inc=1, device_id=(target_row ^ 2, block), device_id_type=MESH)
    pl.semaphore_signal(barrier, inc=1, device_id=(second_row, second), device_id_type=MESH)

    loads[0].wait()
    for u in range(UNITS):
        for g in range(2):
            src[u, :, 128 * g : 128 * g + 128] = l_in[pl.ds(2 * u + g, ROWS, stride=12), :]
    with jax.named_scope("barrier"):
        pl.semaphore_wait(
            barrier, jnp.where(keeps, 10, 11) + jnp.where(stays, 0, 1) + jnp.where(origin == q, 0, 1)
        )

    def remote(source, target, send, recv, device):
        return pltpu.make_async_remote_copy(
            src_ref=source, dst_ref=target, send_sem=send, recv_sem=recv, device_id=device, device_id_type=MESH
        )

    sends = []

    def go(copy):
        copy.start()
        sends.append(copy)

    kinds = (p, beside, below, below ^ 2, above, above ^ 2, opposite, opposite ^ 2)
    kinds = kinds + tuple(kind ^ 1 for kind in kinds)

    where = [pl.ds(pl.multiple_of(ROWS * chunk_at(kind, q), ROWS), ROWS) for kind in kinds]

    def piece(k, kind):
        return xbuf.at[k, where[kind], :]

    def push(k, kind, slot, as_kind, row):
        go(remote(piece(k, kind), piece(k, kind), xg_send.at[k, slot], xg_recv.at[k, as_kind], (row, q)))

    def wait_piece(k, kind):
        remote(piece(k, kind), piece(k, kind), xg_send.at[k, 0], xg_recv.at[k, kind], (other, q)).wait_recv()

    def push_all(k, kind):
        push(k, kind, 2 + kind, 2 + kind, above)
        push(k, kind, 4 + kind, 4 + kind, below)
        push(k, kind, 6 + kind, 6 + kind, opposite)
        push(k, kind, 8 + kind, 8 + kind, other)

    def take_copy(k):
        return remote(src.at[k], taken.at[k], a_send.at[k], a_recv.at[k], (taker, q))

    def land_copy(k, aside):
        rows = pl.ds(pl.multiple_of(ROWS * q, ROWS), ROWS)
        return remote(
            taken.at[k],
            xbuf.at[k, rows, :],
            xg_send.at[k, aside],
            xg_recv.at[k, aside],
            (target_row ^ (2 * aside), block),
        )

    for k in range(UNITS):

        @pl.when(jnp.logical_not(keeps))
        def _():
            take_copy(k).start()

        @pl.when(keeps)
        def _():
            taken[k] = src[k]

    def st_take(k):
        @pl.when(jnp.logical_not(keeps))
        def _():
            take_copy(k).wait_recv()

        @pl.when(jnp.logical_not(stays))
        def _():
            land_copy(k, 0).start()

        go(land_copy(k, 1))

        @pl.when(stays)
        def _():
            xbuf[k, where[0], :] = taken[k]

    def st_prepare(k):
        loads[1].wait()
        a_high[...], a_low[...] = split(a_in[...])
        for n in range(NSUP):

            for h in range(2):

                def put(t, tile, n=n, h=h):
                    e1s[8 * h + t, 8 * n : 8 * n + 8, :] = tile

                pack(src[2 * n + h], put)
        loads[2].wait()
        loads[3].wait()

    def st_own(k):
        @pl.when(origin != q)
        def _():
            wait_piece(k, 0)

        push_all(k, 0)

    def st_second(k):
        wait_piece(k, 1)
        push_all(k, 1)

    def st_forward(k):
        for kind in (2, 4, 3, 5, 6, 7):
            wait_piece(k, kind)
            push(k, kind, 8 + kind, 8 + kind, other)

    across_first = FIRST_ACROSS
    halves = [(0,) if k in across_first else (0, 1) for k in range(UNITS)]

    def steps(k, h, way):
        return 4 if (k + h + way) % 2 == 0 else 3

    def block_rows(k, h, d):
        half = far if k in across_first else h
        return pl.ds(pl.multiple_of(256 * half + ROWS * d, ROWS), ROWS)

    def sent_block(k, h, way, t):
        left = steps(k, h, way) - t
        return (z - left) & 7 if way == 0 else (z + left) & 7

    def send_sum(k, h, way, t):
        go(
            remote(
                pbuf.at[k, block_rows(k, h, sent_block(k, h, way, t)), :],
                rbuf.at[k, h, way, t],
                rs_send.at[k, h, way, t],
                rs_recv.at[k, h, way, t],
                (p, z_down if way == 0 else z_up),
            )
        )

    def wait_sum(k, h, way, t):
        remote(
            rbuf.at[k, h, way, t], rbuf.at[k, h, way, t], rs_send.at[k, h, way, t], rs_recv.at[k, h, way, t], (p, z_up)
        ).wait_recv()

    def mask_of(k, index):
        return s_in[k // 2, index].astype(F32)

    def half_copy(k):
        rows = pl.ds(pl.multiple_of(256 * (1 - far), 256), 256)
        at = across_first.index(k)
        return remote(pbuf.at[k, rows, :], xhalf.at[at], xs_send.at[k], xs_recv.at[k], (p, across))

    def st_product(k):
        for kind in range(8, 16):
            wait_piece(k, kind)
        x_high, x_low = split(xbuf[k] * mask_of(k, q))
        for m in range(4):
            at = slice(128 * m, 128 * m + 128)
            pbuf[k, at, :] = dot(a_high[at, :], x_high) + dot(a_high[at, :], x_low) + dot(a_low[at, :], x_high)
        if k in across_first:
            go(half_copy(k))

    def st_launch(k):
        if k in across_first:
            half_copy(k).wait_recv()
            rows = pl.ds(pl.multiple_of(256 * far, 256), 256)
            pbuf[k, rows, :] = pbuf[k, rows, :] + xhalf[across_first.index(k)]
        for h in halves[k]:
            for way in range(2):
                send_sum(k, h, way, 0)

    def st_sum(k, t):
        for h in halves[k]:
            for way in range(2):
                last = steps(k, h, way) - 1
                if t > last:
                    continue
                wait_sum(k, h, way, t)
                if t < last:
                    rows = block_rows(k, h, sent_block(k, h, way, t + 1))
                    pbuf[k, rows, :] = pbuf[k, rows, :] + rbuf[k, h, way, t]
                    send_sum(k, h, way, t + 1)
        if t == 3:
            for h in halves[k]:
                total = pbuf[k, block_rows(k, h, z), :]
                for way in range(2):
                    total = total + rbuf[k, h, way, steps(k, h, way) - 1]
                sbuf[k, h] = total
            if k not in across_first:
                go(remote(sbuf.at[k, 1 - far], xrec.at[k], xs_send.at[k], xs_recv.at[k], (p, across)))

    core = p & 1
    pair = p - core

    def spread_copy(t):
        tiles = pl.ds(2 * (t >> 1), 2)
        return remote(e1s.at[tiles], e1r.at[p], e1_send.at[t], e1_recv.at[p], (t, q))

    def st_spread(k):
        def one(i, carry):
            spread_copy((p + i) & 15).start()
            return carry

        lax.fori_loop(1, GRID, one, 0)
        e1r[p] = e1s[pl.ds(pair, 2)]

    y_rows = pl.ds(pl.multiple_of(ROWS * p, ROWS), ROWS)

    def y_copy(k, row, slot):
        return remote(ybuf.at[k, y_rows, :], ybuf.at[k, y_rows, :], yg_send.at[k, slot], yg_recv.at[k, p], (row, q))

    def st_panel(k):
        if k in across_first:
            total = sbuf[k, 0]
        else:
            remote(xrec.at[k], xrec.at[k], xs_send.at[k], xs_recv.at[k], (p, across)).wait_recv()
            total = sbuf[k, far] + xrec[k]
        y = total * (-mask_of(k, p))
        ybuf[k, y_rows, :] = y
        for g in range(2):
            y_out[pl.ds(2 * k + g, ROWS, stride=12), :] = y[:, 128 * g : 128 * g + 128]
        near = p - core + k % 2
        for n, turn in enumerate((2, 4, 12, 6, 14, 8, 10)):
            row = (near ^ (turn & 2)) + (turn & 12) & 15
            go(y_copy(k, row, n + 1))

        @pl.when(core != k % 2)
        def _():
            y_copy(k, other, 0).start()

    def st_spread_wait(k):
        def one(i, carry):
            t = (p + i) & 15
            remote(e1r.at[t], e1r.at[t], e1_send.at[t], e1_recv.at[t], (other, q)).wait_recv()
            return carry

        lax.fori_loop(1, GRID, one, 0)

    def e2_copy(n, w, t):
        column = 8 * core + t
        return remote(
            e2s.at[n, w, t], e2r.at[n, q], e2_send.at[n, w, t], e2_recv.at[n, q], (pair + w, column)
        )

    def elsewhere(w, t):
        return jnp.logical_or(pair + w != p, 8 * core + t != q)

    def st_diagonal(n):
        left = []
        for w in range(2):
            turned = e1r[:, w, 8 * n : 8 * n + 8, :].reshape(128, 128).T
            left.append([turned[32 * u : 32 * u + 32, :] for u in range(4)])
        left = [split(jnp.concatenate([left[0][u], left[1][u]], axis=0)) for u in range(4)]
        unit = 2 * n + core

        def one(i, carry):
            row = (p + i) & 15
            rows = pl.ds(pl.multiple_of(ROWS * row, ROWS), ROWS)
            piece = ybuf.at[unit, rows, :]
            remote(piece, piece, yg_send.at[n, 0], yg_recv.at[unit, row], (other, q)).wait_recv()
            return carry

        lax.fori_loop(1, GRID, one, 0)
        y = ybuf[unit].reshape(GRID, 4, 8, COLS)
        total = None
        for u in range(4):
            l_high, l_low = left[u]
            y_high, y_low = split(y[:, u].reshape(128, COLS))
            term = dot(l_high, y_high) + dot(l_high, y_low) + dot(l_low, y_high)
            total = term if total is None else total + term
        for w in range(2):

            def put(t, tile, w=w):
                e2s[n, w, t] = tile

            pack(total[32 * w : 32 * w + 32, :], put)

        def two(i, carry):
            t = (q + i) & 7
            for w in range(2):

                @pl.when(elsewhere(w, t))
                def _():
                    e2_copy(n, w, t).start()

            return carry

        lax.fori_loop(0, 8, two, 0)

        @pl.when(far == core)
        def _():
            e2r[n, q] = e2s[n, core, q & 7]

    def st_result(n):
        def one(i, carry):
            t = (q + i) & 15

            @pl.when(jnp.logical_or(t != q, far != core))
            def _():
                remote(e2r.at[n, t], e2r.at[n, t], e1_send.at[0], e2_recv.at[n, t], (other, q)).wait_recv()

            return carry

        lax.fori_loop(0, GRID, one, 0)
        total = jnp.sum(e2r[n], axis=0)
        parts = [total] + [pltpu.roll(total, 128 - 32 * u, 1) for u in range(1, 4)]
        square = jnp.concatenate(parts, axis=0)
        d_out[n] = piv_in[n] - square[:, :ROWS]

    stages = {
        "take": st_take,
        "prepare": st_prepare,
        "own": st_own,
        "second": st_second,
        "forward": st_forward,
        "product": st_product,
        "launch": st_launch,
        "panel": st_panel,
        "spread": st_spread,
        "arrived": st_spread_wait,
        "diagonal": st_diagonal,
        "result": st_result,
    }
    for t in range(4):
        stages[f"sum{t}"] = lambda k, t=t: st_sum(k, t)
    for name, k in ORDER:
        with jax.named_scope(f"{name}_{k}"):
            stages[name](k)

    for k in range(UNITS):

        @pl.when(jnp.logical_not(keeps))
        def _():
            take_copy(k).wait_send()

        @pl.when(jnp.logical_not(stays))
        def _():
            land_copy(k, 0).wait_send()

        @pl.when(core != k % 2)
        def _():
            y_copy(k, other, 0).wait_send()

    for n in range(NSUP):

        def two(t, carry, n=n):
            for w in range(2):

                @pl.when(elsewhere(w, t))
                def _():
                    e2_copy(n, w, t).wait_send()

            return carry

        lax.fori_loop(0, 8, two, 0)

    def one(i, carry):
        spread_copy((p + i) & 15).wait_send()
        return carry

    lax.fori_loop(1, GRID, one, 0)
    for copy in sends:
        copy.wait_send()


def body(ancestor_inverse, factor_panel, pivot_inverse, structure):
    hbm = pl.BlockSpec(memory_space=pltpu.HBM)
    dma = pltpu.SemaphoreType.DMA
    panel, diagonal = pl.pallas_call(
        kernel,
        out_shape=(
            pltpu.VMEM((ROWS * NSUP * 4, 128), F32),
            pltpu.VMEM(pivot_inverse.shape, F32),
        ),
        in_specs=[hbm] * 4,
        out_specs=(pl.BlockSpec(memory_space=pltpu.VMEM),)*2,
        scratch_shapes=[
            pltpu.VMEM((WIDTH, WIDTH), F32),
            pltpu.VMEM((ROWS * NSUP * 4, 128), F32),
            pltpu.VMEM((NSUP, ROWS, ROWS), F32),
            pltpu.SMEM((NSUP, GRID), jnp.int32),
            pltpu.VMEM((WIDTH, WIDTH), BF16),
            pltpu.VMEM((WIDTH, WIDTH), BF16),
            pltpu.VMEM((UNITS, ROWS, COLS), F32),
            pltpu.VMEM((UNITS, ROWS, COLS), F32),
            pltpu.VMEM((UNITS, WIDTH, COLS), F32),
            pltpu.VMEM((UNITS, WIDTH, COLS), F32),
            pltpu.VMEM((UNITS, 2, 2, 4, ROWS, COLS), F32),
            pltpu.VMEM((UNITS, 2, ROWS, COLS), F32),
            pltpu.VMEM((UNITS, ROWS, COLS), F32),
            pltpu.VMEM((len(FIRST_ACROSS), 256, COLS), F32),
            pltpu.VMEM((UNITS, WIDTH, COLS), F32),
            pltpu.VMEM((GRID, NSUP * 8, 128), F32),
            pltpu.VMEM((GRID, 2, NSUP * 8, 128), F32),
            pltpu.VMEM((NSUP, 2, 8, 8, 128), F32),
            pltpu.VMEM((NSUP, GRID, 8, 128), F32),
            dma((4,)),
            dma((UNITS,)),
            dma((UNITS,)),
            dma((UNITS, 16)),
            dma((UNITS, 16)),
            dma((UNITS, 2, 2, 4)),
            dma((UNITS, 2, 2, 4)),
            dma((UNITS,)),
            dma((UNITS,)),
            dma((UNITS, 8)),
            dma((UNITS, GRID)),
            dma((GRID,)),
            dma((GRID,)),
            dma((NSUP, 2, 8)),
            dma((NSUP, GRID)),
        ],
        compiler_params=pltpu.CompilerParams(
            collective_id=0, has_side_effects=True, vmem_limit_bytes=VMEM_LIMIT
        ),
        name="level",
    )(
        pltpu.with_memory_space_constraint(ancestor_inverse.reshape(WIDTH, WIDTH), pltpu.HBM),
        pltpu.with_memory_space_constraint(factor_panel.reshape(ROWS * NSUP * 4, 128), pltpu.HBM),
        pltpu.with_memory_space_constraint(pivot_inverse, pltpu.HBM),
        pltpu.with_memory_space_constraint(structure.T, pltpu.HBM),
    )
    return panel.reshape(ROWS, 1, NSUP, WIDTH), diagonal


def solution(mesh):
    return jax.shard_map(
        body,
        mesh=mesh,
        in_specs=(
            P("prow", "pcol", None, None),
            P("pcol", "prow", None, None),
            P(None, "prow", "pcol"),
            P(),
        ),
        out_specs=(P("pcol", "prow", None, None), P(None, "prow", "pcol")),
        check_vma=False,
    )
```

```python
import jax
import jax.numpy as jnp
from jax import lax
from jax.experimental import pallas as pl
from jax.experimental.pallas import tpu as pltpu
from jax.sharding import PartitionSpec as P

F32 = jnp.float32
BF16 = jnp.bfloat16
MESH = pl.DeviceIdType.MESH
ROWS = 32
NSUP = 3
WIDTH = 512
GRID = 16
UNITS = 6
COLS = 256
IN_FLIGHT = 3
FIRST_ACROSS = ()


VMEM_LIMIT = 40 * 1024 * 1024


ORDER = (
    ("take", 0), ("prepare", 0), ("take", 1), ("take", 2), ("take", 3), ("take", 4), ("take", 5), ("own", 0),
    ("second", 0), ("own", 1), ("second", 1), ("own", 2), ("second", 2), ("own", 3), ("second", 3),
    ("forward", 0), ("own", 4), ("second", 4), ("product", 0), ("own", 5), ("launch", 0), ("second", 5),
    ("forward", 1), ("product", 1), ("launch", 1), ("forward", 2), ("sum0", 0), ("product", 2), ("launch", 2),
    ("forward", 3), ("sum0", 1), ("sum1", 0), ("product", 3), ("launch", 3), ("forward", 4), ("sum0", 2),
    ("sum1", 1), ("product", 4), ("forward", 5), ("sum2", 0), ("sum0", 3), ("product", 5), ("spread", 0),
    ("sum1", 2), ("sum2", 1), ("sum3", 0), ("launch", 4), ("sum1", 3), ("sum2", 2), ("sum3", 1),
    ("launch", 5), ("panel", 0), ("sum0", 4), ("sum2", 3), ("sum3", 2), ("panel", 1), ("sum0", 5),
    ("sum1", 4), ("sum3", 3), ("panel", 2), ("sum1", 5), ("sum2", 4), ("panel", 3), ("arrived", 0),
    ("diagonal", 0), ("sum3", 4), ("sum2", 5), ("sum3", 5), ("panel", 4), ("diagonal", 1), ("panel", 5),
    ("drain", 0), ("diagonal", 2), ("drain", 1), ("result", 0), ("result", 1), ("result", 2),
)


def split(x):
    high = x.astype(BF16)
    return high, (x - high.astype(F32)).astype(BF16)


def dot(a, b):
    return jnp.dot(a, b, preferred_element_type=F32)


def passing(row, chunk):
    bit = chunk & 1
    turn = 2 * (((row >> 1) ^ (chunk >> 1)) & 1) + (((chunk >> 2) & 1) ^ bit)
    return row ^ (4 * turn + bit)


def landing(row, block, chunk):
    return row ^ (2 * (((block >> 3) ^ (chunk >> 3)) & 1))


def chunk_at(row, block):
    high = ((row >> 1) ^ (block >> 1)) & 1
    low = row & 1
    middle = ((row >> 3) ^ (block >> 3)) & 1
    third = ((row >> 2) ^ block ^ low) & 1
    return block ^ (8 * high + 4 * third + 2 * middle + low)


def pack(y, put):
    lane = lax.broadcasted_iota(jnp.int32, (8, 128), 1) >> 5
    for g in range(y.shape[1] // 128):
        tiles = [y[8 * u : 8 * u + 8, 128 * g : 128 * g + 128] for u in range(4)]
        for h in range(4):
            out = None
            for u in range(4):
                by = (32 * (u - h)) % 128
                moved = pltpu.roll(tiles[u], by, 1) if by else tiles[u]
                out = moved if out is None else jnp.where(lane == u, moved, out)
            put(4 * g + h, out)


def kernel(
    a_hbm, l_hbm, piv_hbm, s_hbm,
    y_out, d_out,
    a_in, l_in, piv_in, s_in, a_high, a_low, src, taken, xbuf, pbuf, rbuf, sbuf, xrec, xhalf, ybuf,
    e1s, e1r, e2s, e2r,
    load_sem, a_send, a_recv, land_send, xg_send, xg_recv, rs_send, rs_recv, xs_send, xs_recv, yg_send, yg_recv,
    e1_send, e1_recv, e2_send, e2_recv,
):
    p = lax.axis_index("prow")
    q = lax.axis_index("pcol")
    z = q & 7
    far = q >> 3

    loads = [
        pltpu.make_async_copy(source, target, load_sem.at[n])
        for n, (source, target) in enumerate(((l_hbm, l_in), (a_hbm, a_in), (s_hbm, s_in), (piv_hbm, piv_in)))
    ]
    for load in loads:
        load.start()

    other = p ^ 1
    beside = p ^ 2
    above = (p + 4) & 15
    below = (p - 4) & 15
    z_up = (q & 8) + ((z + 1) & 7)
    z_down = (q & 8) + ((z - 1) & 7)
    across = q ^ 8

    taker = passing(p, q)
    keeps = taker == p
    block = taker
    target_row = landing(p, block, q)
    stays = block == q
    origin = chunk_at(p, q)
    origin_row = landing(p, q, origin)
    second = chunk_at(beside, q)
    second_row = landing(beside, q, second)

    barrier = pltpu.get_barrier_semaphore()
    opposite = (p + 8) & 15
    for device in (
        (other, q), (beside, q), (above, q), (below, q), (opposite, q), (p, z_up), (p, z_down), (p, across)
    ):
        pl.semaphore_signal(barrier, inc=1, device_id=device, device_id_type=MESH)

    @pl.when(jnp.logical_not(keeps))
    def _():
        pl.semaphore_signal(barrier, inc=1, device_id=(taker, q), device_id_type=MESH)

    @pl.when(jnp.logical_not(stays))
    def _():
        pl.semaphore_signal(barrier, inc=1, device_id=(target_row, block), device_id_type=MESH)

    @pl.when(origin != q)
    def _():
        pl.semaphore_signal(barrier, inc=1, device_id=(origin_row, origin), device_id_type=MESH)

    pl.semaphore_signal(barrier, inc=1, device_id=(target_row ^ 2, block), device_id_type=MESH)
    pl.semaphore_signal(barrier, inc=1, device_id=(second_row, second), device_id_type=MESH)

    loads[0].wait()
    for u in range(UNITS):
        for g in range(2):
            src[u, :, 128 * g : 128 * g + 128] = l_in[pl.ds(2 * u + g, ROWS, stride=12), :]
    with jax.named_scope("barrier"):
        pl.semaphore_wait(
            barrier, jnp.where(keeps, 10, 11) + jnp.where(stays, 0, 1) + jnp.where(origin == q, 0, 1)
        )

    def start(copy):
        copy.start()

    def came(ref, sem):
        remote(ref, ref, sem, sem, (other, q)).wait_recv()

    def went(ref, sem):
        remote(ref, ref, sem, sem, (other, q)).wait_send()

    def remote(source, target, send, recv, device):
        return pltpu.make_async_remote_copy(
            src_ref=source, dst_ref=target, send_sem=send, recv_sem=recv, device_id=device, device_id_type=MESH
        )

    kinds = (p, beside, below, below ^ 2, above, above ^ 2, opposite, opposite ^ 2)
    kinds = kinds + tuple(kind ^ 1 for kind in kinds)

    where = [pl.ds(pl.multiple_of(ROWS * chunk_at(kind, q), ROWS), ROWS) for kind in kinds]

    def piece(k, kind):
        return xbuf.at[k, where[kind], :]

    def push(k, kind, as_kind, row):
        group = as_kind if as_kind < 2 else 2 if as_kind < 6 else 3 if as_kind < 8 else 4
        start(remote(piece(k, kind), piece(k, kind), xg_send.at[0], xg_recv.at[k, group], (row, q)))

    def pieces(k, count):
        return xbuf.at[k, pl.ds(0, ROWS * count), :]

    def push_all(k, kind):
        push(k, kind, 2 + kind, above)
        push(k, kind, 4 + kind, below)
        push(k, kind, 6 + kind, opposite)
        push(k, kind, 8 + kind, other)

    def take_copy(k):
        return remote(src.at[k], taken.at[k], a_send.at[0], a_recv.at[k], (taker, q))

    def land_copy(k, aside):
        rows = pl.ds(pl.multiple_of(ROWS * q, ROWS), ROWS)
        return remote(
            taken.at[k],
            xbuf.at[k, rows, :],
            land_send.at[0] if aside == 0 else xg_send.at[0],
            xg_recv.at[k, aside],
            (target_row ^ (2 * aside), block),
        )

    for k in range(UNITS):

        @pl.when(jnp.logical_not(keeps))
        def _():
            take_copy(k).start()

        @pl.when(keeps)
        def _():
            taken[k] = src[k]

    def st_take(k):
        @pl.when(jnp.logical_not(keeps))
        def _():
            take_copy(k).wait_recv()

        @pl.when(jnp.logical_not(stays))
        def _():
            land_copy(k, 0).start()

        land_copy(k, 1).start()

        @pl.when(stays)
        def _():
            xbuf[k, where[0], :] = taken[k]

    def st_prepare(k):
        loads[1].wait()
        a_high[...], a_low[...] = split(a_in[...])
        for n in range(NSUP):

            for h in range(2):

                def put(t, tile, n=n, h=h):
                    e1s[8 * h + t, 8 * n : 8 * n + 8, :] = tile

                pack(src[2 * n + h], put)
        loads[2].wait()
        loads[3].wait()

    def st_own(k):
        @pl.when(origin != q)
        def _():
            came(pieces(k, 1), xg_recv.at[k, 0])

        push_all(k, 0)

    def st_second(k):
        came(pieces(k, 1), xg_recv.at[k, 1])
        push_all(k, 1)

    def st_forward(k):
        came(pieces(k, 4), xg_recv.at[k, 2])
        for kind in range(2, 6):
            push(k, kind, 8 + kind, other)
        came(pieces(k, 2), xg_recv.at[k, 3])
        for kind in range(6, 8):
            push(k, kind, 8 + kind, other)

    across_first = FIRST_ACROSS
    halves = [(0,) if k in across_first else (0, 1) for k in range(UNITS)]

    def steps(k, h, way):
        return 4 if (k + h + way) % 2 == 0 else 3

    def block_rows(k, h, d):
        half = far if k in across_first else h
        return pl.ds(pl.multiple_of(256 * half + ROWS * d, ROWS), ROWS)

    def sent_block(k, h, way, t):
        left = steps(k, h, way) - t
        return (z - left) & 7 if way == 0 else (z + left) & 7

    def slot(t, way):
        return 2 * t + way if t < 3 else 6

    def send_sum(k, h, way, t):
        start(
            remote(
                pbuf.at[k, block_rows(k, h, sent_block(k, h, way, t)), :],
                rbuf.at[k, h, slot(t, way)],
                rs_send.at[k],
                rs_recv.at[k, h, t],
                (p, z_down if way == 0 else z_up),
            )
        )

    def mask_of(k, index):
        return s_in[k // 2, index].astype(F32)

    def half_copy(k):
        rows = pl.ds(pl.multiple_of(256 * (1 - far), 256), 256)
        at = across_first.index(k)
        return remote(pbuf.at[k, rows, :], xhalf.at[at], xs_send.at[k], xs_recv.at[k], (p, across))

    def st_product(k):
        came(pieces(k, 8), xg_recv.at[k, 4])
        x_high, x_low = split(xbuf[k] * mask_of(k, q))
        for m in range(4):
            at = slice(128 * m, 128 * m + 128)
            pbuf[k, at, :] = dot(a_high[at, :], x_high) + dot(a_high[at, :], x_low) + dot(a_low[at, :], x_high)
        if k in across_first:
            half_copy(k).start()

    def st_launch(k):
        if k in across_first:
            half_copy(k).wait_recv()
            rows = pl.ds(pl.multiple_of(256 * far, 256), 256)
            pbuf[k, rows, :] = pbuf[k, rows, :] + xhalf[across_first.index(k)]
        for h in halves[k]:
            for way in range(2):
                send_sum(k, h, way, 0)

    def st_sum(k, t):
        for h in halves[k]:
            came(rbuf.at[k, h, pl.ds(2 * t, 2 if t < 3 else 1)], rs_recv.at[k, h, t])
            for way in range(2):
                if t < steps(k, h, way) - 1:
                    rows = block_rows(k, h, sent_block(k, h, way, t + 1))
                    pbuf[k, rows, :] = pbuf[k, rows, :] + rbuf[k, h, slot(t, way)]
                    send_sum(k, h, way, t + 1)
        if t == 3:
            for h in halves[k]:
                total = pbuf[k, block_rows(k, h, z), :]
                for way in range(2):
                    total = total + rbuf[k, h, slot(steps(k, h, way) - 1, way)]
                sbuf[k, h] = total
            if k not in across_first:
                start(remote(sbuf.at[k, 1 - far], xrec.at[k], xs_send.at[k], xs_recv.at[k], (p, across)))

    core = p & 1
    pair = p - core

    def spread_copy(t):
        tiles = pl.ds(2 * (t >> 1), 2)
        return remote(e1s.at[tiles], e1r.at[p], e1_send.at[0], e1_recv.at[0], (t, q))

    def st_spread(k):
        def one(i, carry):
            spread_copy((p + i) & 15).start()
            return carry

        lax.fori_loop(1, GRID, one, 0)
        e1r[p] = e1s[pl.ds(pair, 2)]

    y_rows = pl.ds(pl.multiple_of(ROWS * p, ROWS), ROWS)

    def y_copy(k, row):
        return remote(ybuf.at[k, y_rows, :], ybuf.at[k, y_rows, :], yg_send.at[0], yg_recv.at[k], (row, q))

    def st_panel(k):
        if k in across_first:
            total = sbuf[k, 0]
        else:
            came(xrec.at[k], xs_recv.at[k])
            total = sbuf[k, far] + xrec[k]
        y = total * (-mask_of(k, p))
        ybuf[k, y_rows, :] = y
        for g in range(2):
            y_out[pl.ds(2 * k + g, ROWS, stride=12), :] = y[:, 128 * g : 128 * g + 128]
        near = p - core + k % 2
        for turn in (8, 10, 4, 12, 6, 14, 2):
            row = (near ^ (turn & 2)) + (turn & 12) & 15
            y_copy(k, row).start()

        @pl.when(core != k % 2)
        def _():
            y_copy(k, other).start()

    def st_spread_wait(k):
        came(e1r.at[pl.ds(0, GRID - 1)], e1_recv.at[0])

    def e2_copy(n, w, t):
        column = 8 * core + t
        return remote(
            e2s.at[n, w, t], e2r.at[n, q], e2_send.at[0], e2_recv.at[n], (pair + w, column)
        )

    def elsewhere(w, t):
        return jnp.logical_or(pair + w != p, 8 * core + t != q)

    def st_diagonal(n):
        left = []
        for w in range(2):
            turned = e1r[:, w, 8 * n : 8 * n + 8, :].reshape(128, 128).T
            left.append([turned[32 * u : 32 * u + 32, :] for u in range(4)])
        left = [split(jnp.concatenate([left[0][u], left[1][u]], axis=0)) for u in range(4)]
        unit = 2 * n + core

        came(ybuf.at[unit, pl.ds(0, ROWS * (GRID - 1)), :], yg_recv.at[unit])
        y = ybuf[unit].reshape(GRID, 4, 8, COLS)
        total = None
        for u in range(4):
            l_high, l_low = left[u]
            y_high, y_low = split(y[:, u].reshape(128, COLS))
            term = dot(l_high, y_high) + dot(l_high, y_low) + dot(l_low, y_high)
            total = term if total is None else total + term
        for w in range(2):

            def put(t, tile, w=w):
                e2s[n, w, t] = tile

            pack(total[32 * w : 32 * w + 32, :], put)

        def two(i, carry):
            t = (q + i) & 7
            for w in range(2):

                @pl.when(elsewhere(w, t))
                def _():
                    e2_copy(n, w, t).start()

            return carry

        lax.fori_loop(0, 8, two, 0)

        @pl.when(far == core)
        def _():
            e2r[n, q] = e2s[n, core, q & 7]

    def st_result(n):
        @pl.when(far == core)
        def _():
            came(e2r.at[n, pl.ds(0, GRID - 1)], e2_recv.at[n])

        @pl.when(far != core)
        def _():
            came(e2r.at[n], e2_recv.at[n])

        total = jnp.sum(e2r[n], axis=0)
        parts = [total] + [pltpu.roll(total, 128 - 32 * u, 1) for u in range(1, 4)]
        square = jnp.concatenate(parts, axis=0)
        d_out[n] = piv_in[n] - square[:, :ROWS]

    def st_drain(n):
        if n == 0:

            @pl.when(jnp.logical_not(keeps))
            def _():
                went(src, a_send.at[0])

            @pl.when(jnp.logical_not(stays))
            def _():
                went(taken, land_send.at[0])

            went(xbuf.at[:, pl.ds(0, 15 * ROWS), :], xg_send.at[0])
            went(e1r.at[pl.ds(0, GRID - 1)], e1_send.at[0])
            return
        for k in range(UNITS):
            if k in across_first:
                half_copy(k).wait_send()
                went(rbuf.at[k, 0], rs_send.at[k])
            else:
                went(xrec.at[k], xs_send.at[k])
                went(rbuf.at[k], rs_send.at[k])
        went(ybuf.at[:, pl.ds(0, 240), :], yg_send.at[0])

    stages = {
        "drain": st_drain,
        "take": st_take,
        "prepare": st_prepare,
        "own": st_own,
        "second": st_second,
        "forward": st_forward,
        "product": st_product,
        "launch": st_launch,
        "panel": st_panel,
        "spread": st_spread,
        "arrived": st_spread_wait,
        "diagonal": st_diagonal,
        "result": st_result,
    }
    for t in range(4):
        stages[f"sum{t}"] = lambda k, t=t: st_sum(k, t)
    for name, k in ORDER:
        with jax.named_scope(f"{name}_{k}"):
            stages[name](k)

    @pl.when(far == core)
    def _():
        went(e2r.at[:, pl.ds(0, GRID - 1)], e2_send.at[0])

    @pl.when(far != core)
    def _():
        went(e2r, e2_send.at[0])


def body(ancestor_inverse, factor_panel, pivot_inverse, structure):
    hbm = pl.BlockSpec(memory_space=pltpu.HBM)
    dma = pltpu.SemaphoreType.DMA
    panel, diagonal = pl.pallas_call(
        kernel,
        out_shape=(
            pltpu.VMEM((ROWS * NSUP * 4, 128), F32),
            pltpu.VMEM(pivot_inverse.shape, F32),
        ),
        in_specs=[hbm] * 4,
        out_specs=(pl.BlockSpec(memory_space=pltpu.VMEM),)*2,
        scratch_shapes=[
            pltpu.VMEM((WIDTH, WIDTH), F32),
            pltpu.VMEM((ROWS * NSUP * 4, 128), F32),
            pltpu.VMEM((NSUP, ROWS, ROWS), F32),
            pltpu.SMEM((NSUP, GRID), jnp.int32),
            pltpu.VMEM((WIDTH, WIDTH), BF16),
            pltpu.VMEM((WIDTH, WIDTH), BF16),
            pltpu.VMEM((UNITS, ROWS, COLS), F32),
            pltpu.VMEM((UNITS, ROWS, COLS), F32),
            pltpu.VMEM((UNITS, WIDTH, COLS), F32),
            pltpu.VMEM((UNITS, WIDTH, COLS), F32),
            pltpu.VMEM((UNITS, 2, 7, ROWS, COLS), F32),
            pltpu.VMEM((UNITS, 2, ROWS, COLS), F32),
            pltpu.VMEM((UNITS, ROWS, COLS), F32),
            pltpu.VMEM((1, 256, COLS), F32),
            pltpu.VMEM((UNITS, WIDTH, COLS), F32),
            pltpu.VMEM((GRID, NSUP * 8, 128), F32),
            pltpu.VMEM((GRID, 2, NSUP * 8, 128), F32),
            pltpu.VMEM((NSUP, 2, 8, 8, 128), F32),
            pltpu.VMEM((NSUP, GRID, 8, 128), F32),
            dma((4,)),
            dma((1,)),
            dma((UNITS,)),
            dma((1,)),
            dma((1,)),
            dma((UNITS, 5)),
            dma((UNITS,)),
            dma((UNITS, 2, 4)),
            dma((UNITS,)),
            dma((UNITS,)),
            dma((1,)),
            dma((UNITS,)),
            dma((1,)),
            dma((1,)),
            dma((1,)),
            dma((NSUP,)),
        ],
        compiler_params=pltpu.CompilerParams(
            collective_id=0, has_side_effects=True, vmem_limit_bytes=VMEM_LIMIT
        ),
        name="level",
    )(
        pltpu.with_memory_space_constraint(ancestor_inverse.reshape(WIDTH, WIDTH), pltpu.HBM),
        pltpu.with_memory_space_constraint(factor_panel.reshape(ROWS * NSUP * 4, 128), pltpu.HBM),
        pltpu.with_memory_space_constraint(pivot_inverse, pltpu.HBM),
        pltpu.with_memory_space_constraint(structure.T, pltpu.HBM),
    )
    return panel.reshape(ROWS, 1, NSUP, WIDTH), diagonal


def solution(mesh):
    return jax.shard_map(
        body,
        mesh=mesh,
        in_specs=(
            P("prow", "pcol", None, None),
            P("pcol", "prow", None, None),
            P(None, "prow", "pcol"),
            P(),
        ),
        out_specs=(P("pcol", "prow", None, None), P(None, "prow", "pcol")),
        check_vma=False,
    )
```

```python
import jax
import jax.numpy as jnp
from jax import lax
from jax.experimental import pallas as pl
from jax.experimental.pallas import tpu as pltpu
from jax.sharding import PartitionSpec as P

F32 = jnp.float32
BF16 = jnp.bfloat16
MESH = pl.DeviceIdType.MESH
ROWS = 32
NSUP = 3
WIDTH = 512
GRID = 16
UNITS = 6
COLS = 256
IN_FLIGHT = 3
FIRST_ACROSS = (1, 4)


VMEM_LIMIT = 40 * 1024 * 1024


ORDER = (
    ("take", 0), ("prepare", 0), ("take", 1), ("take", 2), ("take", 3), ("take", 4), ("take", 5), ("own", 0),
    ("second", 0), ("own", 1), ("second", 1), ("own", 2), ("second", 2), ("own", 3), ("second", 3),
    ("forward", 0), ("own", 4), ("second", 4), ("product", 0), ("own", 5), ("launch", 0), ("second", 5),
    ("forward", 1), ("product", 1), ("forward", 2), ("sum0", 0), ("product", 2), ("launch", 2),
    ("forward", 3), ("sum1", 0), ("product", 3), ("launch", 3), ("forward", 4), ("sum0", 2), ("sum2", 0),
    ("product", 4), ("forward", 5), ("sum0", 3), ("launch", 1), ("sum1", 2), ("product", 5), ("sum3", 0),
    ("launch", 5), ("spread", 0), ("sum1", 3), ("sum0", 1), ("sum2", 2), ("sum0", 5), ("sum2", 3),
    ("sum1", 1), ("panel", 0), ("sum3", 2), ("launch", 4), ("sum1", 5), ("sum3", 3), ("sum2", 1), ("sum0", 4),
    ("sum2", 5), ("sum3", 1), ("panel", 1), ("sum1", 4), ("sum3", 5), ("sum2", 4), ("panel", 2), ("panel", 3),
    ("sum3", 4), ("panel", 4), ("arrived", 0), ("diagonal", 0), ("panel", 5), ("drain", 0), ("diagonal", 1),
    ("diagonal", 2), ("drain", 1), ("result", 0), ("result", 1), ("result", 2),
)


def split(x):
    high = x.astype(BF16)
    return high, (x - high.astype(F32)).astype(BF16)


def dot(a, b):
    return jnp.dot(a, b, preferred_element_type=F32)


def passing(row, chunk):
    bit = chunk & 1
    turn = 2 * (((row >> 1) ^ (chunk >> 1)) & 1) + (((chunk >> 2) & 1) ^ bit)
    return row ^ (4 * turn + bit)


def landing(row, block, chunk):
    return row ^ (2 * (((block >> 3) ^ (chunk >> 3)) & 1))


def chunk_at(row, block):
    high = ((row >> 1) ^ (block >> 1)) & 1
    low = row & 1
    middle = ((row >> 3) ^ (block >> 3)) & 1
    third = ((row >> 2) ^ block ^ low) & 1
    return block ^ (8 * high + 4 * third + 2 * middle + low)


def pack(y, put):
    lane = lax.broadcasted_iota(jnp.int32, (8, 128), 1) >> 5
    for g in range(y.shape[1] // 128):
        tiles = [y[8 * u : 8 * u + 8, 128 * g : 128 * g + 128] for u in range(4)]
        for h in range(4):
            out = None
            for u in range(4):
                by = (32 * (u - h)) % 128
                moved = pltpu.roll(tiles[u], by, 1) if by else tiles[u]
                out = moved if out is None else jnp.where(lane == u, moved, out)
            put(4 * g + h, out)


def kernel(
    a_hbm, l_hbm, piv_hbm, s_hbm,
    y_out, d_out,
    a_in, l_in, piv_in, s_in, a_high, a_low, src, taken, xbuf, pbuf, rbuf, sbuf, xrec, xhalf, ystage, yq, l_high, l_low,
    e1s, e1r, e2s, e2r,
    load_sem, a_send, a_recv, land_send, xg_send, xg_recv, rs_send, rs_recv, xs_send, xs_recv, yg_send, yg_recv,
    e1_send, e1_recv, e2_send, e2_recv,
):
    p = lax.axis_index("prow")
    q = lax.axis_index("pcol")
    z = q & 7
    far = q >> 3

    loads = [
        pltpu.make_async_copy(source, target, load_sem.at[n])
        for n, (source, target) in enumerate(((l_hbm, l_in), (a_hbm, a_in), (s_hbm, s_in), (piv_hbm, piv_in)))
    ]
    for load in loads:
        load.start()

    other = p ^ 1
    beside = p ^ 2
    above = (p + 4) & 15
    below = (p - 4) & 15
    z_up = (q & 8) + ((z + 1) & 7)
    z_down = (q & 8) + ((z - 1) & 7)
    across = q ^ 8

    taker = passing(p, q)
    keeps = taker == p
    block = taker
    target_row = landing(p, block, q)
    stays = block == q
    origin = chunk_at(p, q)
    origin_row = landing(p, q, origin)
    second = chunk_at(beside, q)
    second_row = landing(beside, q, second)

    barrier = pltpu.get_barrier_semaphore()
    opposite = (p + 8) & 15
    for device in (
        (other, q), (beside, q), (above, q), (below, q), (opposite, q), (p, z_up), (p, z_down), (p, across)
    ):
        pl.semaphore_signal(barrier, inc=1, device_id=device, device_id_type=MESH)

    @pl.when(jnp.logical_not(keeps))
    def _():
        pl.semaphore_signal(barrier, inc=1, device_id=(taker, q), device_id_type=MESH)

    @pl.when(jnp.logical_not(stays))
    def _():
        pl.semaphore_signal(barrier, inc=1, device_id=(target_row, block), device_id_type=MESH)

    @pl.when(origin != q)
    def _():
        pl.semaphore_signal(barrier, inc=1, device_id=(origin_row, origin), device_id_type=MESH)

    pl.semaphore_signal(barrier, inc=1, device_id=(target_row ^ 2, block), device_id_type=MESH)
    pl.semaphore_signal(barrier, inc=1, device_id=(second_row, second), device_id_type=MESH)

    loads[0].wait()
    for u in range(UNITS):
        for g in range(2):
            src[u, :, 128 * g : 128 * g + 128] = l_in[pl.ds(2 * u + g, ROWS, stride=12), :]
    with jax.named_scope("barrier"):
        pl.semaphore_wait(
            barrier, jnp.where(keeps, 10, 11) + jnp.where(stays, 0, 1) + jnp.where(origin == q, 0, 1)
        )

    def start(copy):
        copy.start()

    def came(ref, sem):
        remote(ref, ref, sem, sem, (other, q)).wait_recv()

    def went(ref, sem):
        remote(ref, ref, sem, sem, (other, q)).wait_send()

    def remote(source, target, send, recv, device):
        return pltpu.make_async_remote_copy(
            src_ref=source, dst_ref=target, send_sem=send, recv_sem=recv, device_id=device, device_id_type=MESH
        )

    kinds = (p, beside, below, below ^ 2, above, above ^ 2, opposite, opposite ^ 2)
    kinds = kinds + tuple(kind ^ 1 for kind in kinds)

    where = [pl.ds(pl.multiple_of(ROWS * chunk_at(kind, q), ROWS), ROWS) for kind in kinds]

    def piece(k, kind):
        return xbuf.at[k, where[kind], :]

    def push(k, kind, as_kind, row):
        group = as_kind if as_kind < 2 else 2 if as_kind < 6 else 3 if as_kind < 8 else 4
        start(remote(piece(k, kind), piece(k, kind), xg_send.at[0], xg_recv.at[k, group], (row, q)))

    def pieces(k, count):
        return xbuf.at[k, pl.ds(0, ROWS * count), :]

    def push_all(k, kind):
        push(k, kind, 2 + kind, above)
        push(k, kind, 4 + kind, below)
        push(k, kind, 6 + kind, opposite)
        push(k, kind, 8 + kind, other)

    def take_copy(k):
        return remote(src.at[k], taken.at[k], a_send.at[0], a_recv.at[k], (taker, q))

    def land_copy(k, aside):
        rows = pl.ds(pl.multiple_of(ROWS * q, ROWS), ROWS)
        return remote(
            taken.at[k],
            xbuf.at[k, rows, :],
            land_send.at[0] if aside == 0 else xg_send.at[0],
            xg_recv.at[k, aside],
            (target_row ^ (2 * aside), block),
        )

    for k in range(UNITS):

        @pl.when(jnp.logical_not(keeps))
        def _():
            take_copy(k).start()

        @pl.when(keeps)
        def _():
            taken[k] = src[k]

    def st_take(k):
        @pl.when(jnp.logical_not(keeps))
        def _():
            take_copy(k).wait_recv()

        @pl.when(jnp.logical_not(stays))
        def _():
            land_copy(k, 0).start()

        land_copy(k, 1).start()

        @pl.when(stays)
        def _():
            xbuf[k, where[0], :] = taken[k]

    def st_prepare(k):
        loads[1].wait()
        a_high[...], a_low[...] = split(a_in[...])
        for n in range(NSUP):
            for g in range(4):
                e1s[g, n] = src[2 * n + g // 2, :, 128 * (g % 2) : 128 * (g % 2) + 128]
        loads[2].wait()
        loads[3].wait()

    def st_own(k):
        @pl.when(origin != q)
        def _():
            came(pieces(k, 1), xg_recv.at[k, 0])

        push_all(k, 0)

    def st_second(k):
        came(pieces(k, 1), xg_recv.at[k, 1])
        push_all(k, 1)

    def st_forward(k):
        came(pieces(k, 4), xg_recv.at[k, 2])
        for kind in range(2, 6):
            push(k, kind, 8 + kind, other)
        came(pieces(k, 2), xg_recv.at[k, 3])
        for kind in range(6, 8):
            push(k, kind, 8 + kind, other)

    across_first = FIRST_ACROSS
    halves = [(0,) if k in across_first else (0, 1) for k in range(UNITS)]

    def steps(k, h, way):
        return 4 if (k + h + way) % 2 == 0 else 3

    def block_rows(k, h, d):
        half = far if k in across_first else h
        return pl.ds(pl.multiple_of(256 * half + ROWS * d, ROWS), ROWS)

    def sent_block(k, h, way, t):
        left = steps(k, h, way) - t
        return (z - left) & 7 if way == 0 else (z + left) & 7

    def slot(t, way):
        return 2 * t + way if t < 3 else 6

    def send_sum(k, h, way, t):
        start(
            remote(
                pbuf.at[k, block_rows(k, h, sent_block(k, h, way, t)), :],
                rbuf.at[k, h, slot(t, way)],
                rs_send.at[k],
                rs_recv.at[k, h, t],
                (p, z_down if way == 0 else z_up),
            )
        )

    def mask_of(k, index):
        return s_in[k // 2, index].astype(F32)

    def half_copy(k):
        rows = pl.ds(pl.multiple_of(256 * (1 - far), 256), 256)
        at = across_first.index(k)
        return remote(pbuf.at[k, rows, :], xhalf.at[at], xs_send.at[k], xs_recv.at[k], (p, across))

    def st_product(k):
        came(pieces(k, 8), xg_recv.at[k, 4])
        x_high, x_low = split(xbuf[k] * mask_of(k, q))
        for m in range(4):
            at = slice(128 * m, 128 * m + 128)
            pbuf[k, at, :] = dot(a_high[at, :], x_high) + dot(a_high[at, :], x_low) + dot(a_low[at, :], x_high)
        if k in across_first:
            half_copy(k).start()

    def st_launch(k):
        if k in across_first:
            half_copy(k).wait_recv()
            rows = pl.ds(pl.multiple_of(256 * far, 256), 256)
            pbuf[k, rows, :] = pbuf[k, rows, :] + xhalf[across_first.index(k)]
        for h in halves[k]:
            for way in range(2):
                send_sum(k, h, way, 0)

    def st_sum(k, t):
        for h in halves[k]:
            came(rbuf.at[k, h, pl.ds(2 * t, 2 if t < 3 else 1)], rs_recv.at[k, h, t])
            for way in range(2):
                if t < steps(k, h, way) - 1:
                    rows = block_rows(k, h, sent_block(k, h, way, t + 1))
                    pbuf[k, rows, :] = pbuf[k, rows, :] + rbuf[k, h, slot(t, way)]
                    send_sum(k, h, way, t + 1)
        if t == 3:
            for h in halves[k]:
                total = pbuf[k, block_rows(k, h, z), :]
                for way in range(2):
                    total = total + rbuf[k, h, slot(steps(k, h, way) - 1, way)]
                sbuf[k, h] = total
            if k not in across_first:
                start(remote(sbuf.at[k, 1 - far], xrec.at[k], xs_send.at[k], xs_recv.at[k], (p, across)))

    core = p & 1
    side = (p >> 1) & 1
    mine = p & 3

    def spread_copy(t):
        return remote(e1s.at[t >> 2], e1r.at[p], e1_send.at[0], e1_recv.at[0], (t, q))

    def st_spread(k):
        def one(i, carry):
            spread_copy((p + i) & 15).start()
            return carry

        lax.fori_loop(1, GRID, one, 0)
        e1r[p] = e1s[p >> 2]

    y_rows = pl.ds(pl.multiple_of(ROWS * p, ROWS), ROWS)

    def y_copy(k, row, c):
        return remote(
            ystage.at[k, :, pl.ds(128 * c, 128)], yq.at[k // 2, y_rows, :], yg_send.at[0], yg_recv.at[k // 2], (row, q)
        )

    def st_panel(k):
        if k in across_first:
            total = sbuf[k, 0]
        else:
            came(xrec.at[k], xs_recv.at[k])
            total = sbuf[k, far] + xrec[k]
        y = total * (-mask_of(k, p))
        ystage[k] = y
        for g in range(2):
            y_out[pl.ds(2 * k + g, ROWS, stride=12), :] = y[:, 128 * g : 128 * g + 128]
        for up in (8, 4, 12, 0):
            for c in range(2):
                row = 4 * (((p + up) & 15) >> 2) + 2 * (k % 2) + c
                if up:
                    y_copy(k, row, c).start()
                else:

                    @pl.when(mine != 2 * (k % 2) + c)
                    def _():
                        y_copy(k, row, c).start()

                    @pl.when(mine == 2 * (k % 2) + c)
                    def _():
                        yq[k // 2, y_rows, :] = y[:, 128 * c : 128 * c + 128]

    def st_spread_wait(k):
        came(e1r.at[pl.ds(0, GRID - 1)], e1_recv.at[0])
        for n in range(NSUP):
            l_high[n], l_low[n] = split(e1r[:, n].reshape(WIDTH, 128).T)

    same = mine == (q >> 2)

    def e2_copy(n, w, t):
        return remote(
            e2s.at[n, w, t], e2r.at[n, q], e2_send.at[0], e2_recv.at[n], (p - mine + w, 4 * mine + t)
        )

    def st_diagonal(n):
        came(yq.at[n, pl.ds(0, ROWS * (GRID - 1)), :], yg_recv.at[n])
        y_high, y_low = split(yq[n])
        total = dot(l_high[n], y_high) + dot(l_high[n], y_low) + dot(l_low[n], y_high)
        for w in range(4):

            def put(t, tile, w=w):
                e2s[n, w, t] = tile

            pack(total[32 * w : 32 * w + 32, :], put)
        for w in range(4):
            for t in range(4):

                @pl.when(jnp.logical_or(mine != w, 4 * mine + t != q))
                def _():
                    e2_copy(n, w, t).start()

        @pl.when(same)
        def _():
            e2r[n, q] = e2s[n, mine, q & 3]

    def st_result(n):
        @pl.when(same)
        def _():
            came(e2r.at[n, pl.ds(0, GRID - 1)], e2_recv.at[n])

        @pl.when(jnp.logical_not(same))
        def _():
            came(e2r.at[n], e2_recv.at[n])

        total = jnp.sum(e2r[n], axis=0)
        parts = [total] + [pltpu.roll(total, 128 - 32 * u, 1) for u in range(1, 4)]
        square = jnp.concatenate(parts, axis=0)
        d_out[n] = piv_in[n] - square[:, :ROWS]

    def st_drain(n):
        if n == 0:

            @pl.when(jnp.logical_not(keeps))
            def _():
                went(src, a_send.at[0])

            @pl.when(jnp.logical_not(stays))
            def _():
                went(taken, land_send.at[0])

            went(xbuf.at[:, pl.ds(0, 15 * ROWS), :], xg_send.at[0])
            went(e1r.at[pl.ds(0, GRID - 1)], e1_send.at[0])
            return
        for k in range(UNITS):
            if k in across_first:
                half_copy(k).wait_send()
                went(rbuf.at[k, 0], rs_send.at[k])
            else:
                went(xrec.at[k], xs_send.at[k])
                went(rbuf.at[k], rs_send.at[k])
        went(yq.at[:, pl.ds(0, ROWS * (GRID - 1)), :], yg_send.at[0])

    stages = {
        "drain": st_drain,
        "take": st_take,
        "prepare": st_prepare,
        "own": st_own,
        "second": st_second,
        "forward": st_forward,
        "product": st_product,
        "launch": st_launch,
        "panel": st_panel,
        "spread": st_spread,
        "arrived": st_spread_wait,
        "diagonal": st_diagonal,
        "result": st_result,
    }
    for t in range(4):
        stages[f"sum{t}"] = lambda k, t=t: st_sum(k, t)
    for name, k in ORDER:
        with jax.named_scope(f"{name}_{k}"):
            stages[name](k)

    @pl.when(same)
    def _():
        went(e2r.at[:, pl.ds(0, GRID - 1)], e2_send.at[0])

    @pl.when(jnp.logical_not(same))
    def _():
        went(e2r, e2_send.at[0])


def body(ancestor_inverse, factor_panel, pivot_inverse, structure):
    hbm = pl.BlockSpec(memory_space=pltpu.HBM)
    dma = pltpu.SemaphoreType.DMA
    panel, diagonal = pl.pallas_call(
        kernel,
        out_shape=(
            pltpu.VMEM((ROWS * NSUP * 4, 128), F32),
            pltpu.VMEM(pivot_inverse.shape, F32),
        ),
        in_specs=[hbm] * 4,
        out_specs=(pl.BlockSpec(memory_space=pltpu.VMEM),)*2,
        scratch_shapes=[
            pltpu.VMEM((WIDTH, WIDTH), F32),
            pltpu.VMEM((ROWS * NSUP * 4, 128), F32),
            pltpu.VMEM((NSUP, ROWS, ROWS), F32),
            pltpu.SMEM((NSUP, GRID), jnp.int32),
            pltpu.VMEM((WIDTH, WIDTH), BF16),
            pltpu.VMEM((WIDTH, WIDTH), BF16),
            pltpu.VMEM((UNITS, ROWS, COLS), F32),
            pltpu.VMEM((UNITS, ROWS, COLS), F32),
            pltpu.VMEM((UNITS, WIDTH, COLS), F32),
            pltpu.VMEM((UNITS, WIDTH, COLS), F32),
            pltpu.VMEM((UNITS, 2, 7, ROWS, COLS), F32),
            pltpu.VMEM((UNITS, 2, ROWS, COLS), F32),
            pltpu.VMEM((UNITS, ROWS, COLS), F32),
            pltpu.VMEM((len(FIRST_ACROSS), 256, COLS), F32),
            pltpu.VMEM((UNITS, ROWS, COLS), F32),
            pltpu.VMEM((NSUP, WIDTH, 128), F32),
            pltpu.VMEM((NSUP, 128, WIDTH), BF16),
            pltpu.VMEM((NSUP, 128, WIDTH), BF16),
            pltpu.VMEM((4, NSUP, ROWS, 128), F32),
            pltpu.VMEM((GRID, NSUP, ROWS, 128), F32),
            pltpu.VMEM((NSUP, 4, 4, 8, 128), F32),
            pltpu.VMEM((NSUP, GRID, 8, 128), F32),
            dma((4,)),
            dma((1,)),
            dma((UNITS,)),
            dma((1,)),
            dma((1,)),
            dma((UNITS, 5)),
            dma((UNITS,)),
            dma((UNITS, 2, 4)),
            dma((UNITS,)),
            dma((UNITS,)),
            dma((1,)),
            dma((NSUP,)),
            dma((1,)),
            dma((1,)),
            dma((1,)),
            dma((NSUP,)),
        ],
        compiler_params=pltpu.CompilerParams(
            collective_id=0, has_side_effects=True, vmem_limit_bytes=VMEM_LIMIT
        ),
        name="level",
    )(
        pltpu.with_memory_space_constraint(ancestor_inverse.reshape(WIDTH, WIDTH), pltpu.HBM),
        pltpu.with_memory_space_constraint(factor_panel.reshape(ROWS * NSUP * 4, 128), pltpu.HBM),
        pltpu.with_memory_space_constraint(pivot_inverse, pltpu.HBM),
        pltpu.with_memory_space_constraint(structure.T, pltpu.HBM),
    )
    return panel.reshape(ROWS, 1, NSUP, WIDTH), diagonal


def solution(mesh):
    return jax.shard_map(
        body,
        mesh=mesh,
        in_specs=(
            P("prow", "pcol", None, None),
            P("pcol", "prow", None, None),
            P(None, "prow", "pcol"),
            P(),
        ),
        out_specs=(P("pcol", "prow", None, None), P(None, "prow", "pcol")),
        check_vma=False,
    )
```

```python
import jax
import jax.numpy as jnp
from jax import lax
from jax.experimental import pallas as pl
from jax.experimental.pallas import tpu as pltpu
from jax.sharding import PartitionSpec as P

F32 = jnp.float32
BF16 = jnp.bfloat16
MESH = pl.DeviceIdType.MESH
ROWS = 32
NSUP = 3
WIDTH = 512
GRID = 16
UNITS = 12
COLS = 128
IN_FLIGHT = 3
FIRST_ACROSS = (2, 4, 7, 9)


VMEM_LIMIT = 40 * 1024 * 1024


ORDER = (
    ("take", 0), ("prepare", 0), ("take", 1), ("take", 2), ("take", 3), ("take", 4), ("take", 5), ("take", 6),
    ("take", 7), ("take", 8), ("take", 9), ("take", 10), ("take", 11), ("own", 0), ("second", 0), ("own", 1),
    ("second", 1), ("own", 2), ("second", 2), ("own", 3), ("second", 3), ("own", 4), ("second", 4),
    ("own", 5), ("forward", 0), ("second", 5), ("own", 6), ("second", 6), ("own", 7), ("forward", 1),
    ("product", 0), ("second", 7), ("own", 8), ("launch", 0), ("second", 8), ("own", 9), ("forward", 2),
    ("product", 1), ("second", 9), ("own", 10), ("launch", 1), ("second", 10), ("own", 11), ("forward", 3),
    ("product", 2), ("sum0", 0), ("second", 11), ("forward", 4), ("product", 3), ("sum0", 1), ("launch", 3),
    ("forward", 5), ("product", 4), ("sum1", 0), ("forward", 6), ("product", 5), ("sum1", 1), ("launch", 5),
    ("sum0", 3), ("forward", 7), ("product", 6), ("sum2", 0), ("launch", 6), ("launch", 2), ("forward", 8),
    ("product", 7), ("sum2", 1), ("sum0", 5), ("forward", 9), ("product", 8), ("sum1", 3), ("launch", 8),
    ("launch", 4), ("sum3", 0), ("forward", 10), ("sum0", 6), ("product", 9), ("sum0", 2), ("sum3", 1),
    ("forward", 11), ("sum1", 5), ("product", 10), ("launch", 10), ("sum2", 3), ("sum0", 8), ("product", 11),
    ("sum0", 4), ("launch", 11), ("spread", 0), ("panel", 0), ("sum1", 6), ("sum1", 2), ("sum2", 5),
    ("sum0", 10), ("sum3", 3), ("launch", 7), ("sum1", 8), ("panel", 1), ("sum1", 4), ("sum0", 11),
    ("sum2", 6), ("sum2", 2), ("sum3", 5), ("launch", 9), ("sum1", 10), ("sum0", 7), ("sum2", 8), ("sum2", 4),
    ("sum1", 11), ("sum3", 6), ("sum3", 2), ("panel", 2), ("sum0", 9), ("sum2", 10), ("sum1", 7), ("sum3", 8),
    ("sum3", 4), ("panel", 4), ("sum2", 11), ("sum1", 9), ("sum3", 10), ("panel", 3), ("sum2", 7),
    ("panel", 5), ("sum3", 11), ("panel", 6), ("sum2", 9), ("sum3", 7), ("panel", 8), ("panel", 7),
    ("panel", 10), ("sum3", 9), ("panel", 9), ("arrived", 0), ("diagonal", 0), ("panel", 11), ("drain", 0),
    ("diagonal", 1), ("diagonal", 2), ("drain", 1), ("result", 0), ("result", 1), ("result", 2),
)


def split(x):
    high = x.astype(BF16)
    return high, (x - high.astype(F32)).astype(BF16)


def dot(a, b):
    return jnp.dot(a, b, preferred_element_type=F32)


def passing(row, chunk):
    bit = chunk & 1
    turn = 2 * (((row >> 1) ^ (chunk >> 1)) & 1) + (((chunk >> 2) & 1) ^ bit)
    return row ^ (4 * turn + bit)


def landing(row, block, chunk):
    return row ^ (2 * (((block >> 3) ^ (chunk >> 3)) & 1))


def chunk_at(row, block):
    high = ((row >> 1) ^ (block >> 1)) & 1
    low = row & 1
    middle = ((row >> 3) ^ (block >> 3)) & 1
    third = ((row >> 2) ^ block ^ low) & 1
    return block ^ (8 * high + 4 * third + 2 * middle + low)


def pack(y, put):
    lane = lax.broadcasted_iota(jnp.int32, (8, 128), 1) >> 5
    for g in range(y.shape[1] // 128):
        tiles = [y[8 * u : 8 * u + 8, 128 * g : 128 * g + 128] for u in range(4)]
        for h in range(4):
            out = None
            for u in range(4):
                by = (32 * (u - h)) % 128
                moved = pltpu.roll(tiles[u], by, 1) if by else tiles[u]
                out = moved if out is None else jnp.where(lane == u, moved, out)
            put(4 * g + h, out)


def kernel(
    a_hbm, l_hbm, piv_hbm, s_hbm,
    y_out, d_out,
    a_in, l_in, piv_in, s_in, a_high, a_low, src, taken, xbuf, pbuf, rbuf, sbuf, xrec, xhalf, ystage, yq, l_high, l_low,
    e1s, e1r, e2s, e2r,
    load_sem, a_send, a_recv, land_send, xg_send, xg_recv, rs_send, rs_recv, xs_send, xs_recv, yg_send, yg_recv,
    e1_send, e1_recv, e2_send, e2_recv,
):
    p = lax.axis_index("prow")
    q = lax.axis_index("pcol")
    z = q & 7
    far = q >> 3

    loads = [
        pltpu.make_async_copy(source, target, load_sem.at[n])
        for n, (source, target) in enumerate(((l_hbm, l_in), (a_hbm, a_in), (s_hbm, s_in), (piv_hbm, piv_in)))
    ]
    for load in loads:
        load.start()

    other = p ^ 1
    beside = p ^ 2
    above = (p + 4) & 15
    below = (p - 4) & 15
    z_up = (q & 8) + ((z + 1) & 7)
    z_down = (q & 8) + ((z - 1) & 7)
    across = q ^ 8

    taker = passing(p, q)
    keeps = taker == p
    block = taker
    target_row = landing(p, block, q)
    stays = block == q
    origin = chunk_at(p, q)
    origin_row = landing(p, q, origin)
    second = chunk_at(beside, q)
    second_row = landing(beside, q, second)

    barrier = pltpu.get_barrier_semaphore()
    opposite = (p + 8) & 15
    for device in (
        (other, q), (beside, q), (above, q), (below, q), (opposite, q), (p, z_up), (p, z_down), (p, across)
    ):
        pl.semaphore_signal(barrier, inc=1, device_id=device, device_id_type=MESH)

    @pl.when(jnp.logical_not(keeps))
    def _():
        pl.semaphore_signal(barrier, inc=1, device_id=(taker, q), device_id_type=MESH)

    @pl.when(jnp.logical_not(stays))
    def _():
        pl.semaphore_signal(barrier, inc=1, device_id=(target_row, block), device_id_type=MESH)

    @pl.when(origin != q)
    def _():
        pl.semaphore_signal(barrier, inc=1, device_id=(origin_row, origin), device_id_type=MESH)

    pl.semaphore_signal(barrier, inc=1, device_id=(target_row ^ 2, block), device_id_type=MESH)
    pl.semaphore_signal(barrier, inc=1, device_id=(second_row, second), device_id_type=MESH)

    loads[0].wait()
    for u in range(UNITS):
        src[u] = l_in[pl.ds(u, ROWS, stride=12), :]
    with jax.named_scope("barrier"):
        pl.semaphore_wait(
            barrier, jnp.where(keeps, 10, 11) + jnp.where(stays, 0, 1) + jnp.where(origin == q, 0, 1)
        )

    def start(copy):
        copy.start()

    def came(ref, sem):
        remote(ref, ref, sem, sem, (other, q)).wait_recv()

    def went(ref, sem):
        remote(ref, ref, sem, sem, (other, q)).wait_send()

    def remote(source, target, send, recv, device):
        return pltpu.make_async_remote_copy(
            src_ref=source, dst_ref=target, send_sem=send, recv_sem=recv, device_id=device, device_id_type=MESH
        )

    kinds = (p, beside, below, below ^ 2, above, above ^ 2, opposite, opposite ^ 2)
    kinds = kinds + tuple(kind ^ 1 for kind in kinds)

    where = [pl.ds(pl.multiple_of(ROWS * chunk_at(kind, q), ROWS), ROWS) for kind in kinds]

    def piece(k, kind):
        return xbuf.at[k, where[kind], :]

    def push(k, kind, as_kind, row):
        group = as_kind if as_kind < 2 else 2 if as_kind < 6 else 3 if as_kind < 8 else 4
        start(remote(piece(k, kind), piece(k, kind), xg_send.at[0], xg_recv.at[k, group], (row, q)))

    def pieces(k, count):
        return xbuf.at[k, pl.ds(0, ROWS * count), :]

    def push_all(k, kind):
        push(k, kind, 6 + kind, opposite)
        push(k, kind, 2 + kind, above)
        push(k, kind, 4 + kind, below)
        push(k, kind, 8 + kind, other)

    def take_copy(k):
        return remote(src.at[k], taken.at[k], a_send.at[0], a_recv.at[k], (taker, q))

    def land_copy(k, aside):
        rows = pl.ds(pl.multiple_of(ROWS * q, ROWS), ROWS)
        return remote(
            taken.at[k],
            xbuf.at[k, rows, :],
            land_send.at[0] if aside == 0 else xg_send.at[0],
            xg_recv.at[k, aside],
            (target_row ^ (2 * aside), block),
        )

    for k in range(UNITS):

        @pl.when(jnp.logical_not(keeps))
        def _():
            take_copy(k).start()

        @pl.when(keeps)
        def _():
            taken[k] = src[k]

    def st_take(k):
        @pl.when(jnp.logical_not(keeps))
        def _():
            take_copy(k).wait_recv()

        @pl.when(jnp.logical_not(stays))
        def _():
            land_copy(k, 0).start()

        land_copy(k, 1).start()

        @pl.when(stays)
        def _():
            xbuf[k, where[0], :] = taken[k]

    def st_prepare(k):
        loads[1].wait()
        a_high[...], a_low[...] = split(a_in[...])
        for n in range(NSUP):
            for g in range(4):
                e1s[g, n] = src[4 * n + g]
        loads[2].wait()
        loads[3].wait()

    def st_own(k):
        @pl.when(origin != q)
        def _():
            came(pieces(k, 1), xg_recv.at[k, 0])

        push_all(k, 0)

    def st_second(k):
        came(pieces(k, 1), xg_recv.at[k, 1])
        push_all(k, 1)

    def st_forward(k):
        came(pieces(k, 4), xg_recv.at[k, 2])
        for kind in range(2, 6):
            push(k, kind, 8 + kind, other)
        came(pieces(k, 2), xg_recv.at[k, 3])
        for kind in range(6, 8):
            push(k, kind, 8 + kind, other)

    across_first = FIRST_ACROSS
    halves = [(0,) if k in across_first else (0, 1) for k in range(UNITS)]

    def steps(k, h, way):
        return 4 if (k + h + way) % 2 == 0 else 3

    def block_rows(k, h, d):
        half = far if k in across_first else h
        return pl.ds(pl.multiple_of(256 * half + ROWS * d, ROWS), ROWS)

    def sent_block(k, h, way, t):
        left = steps(k, h, way) - t
        return (z - left) & 7 if way == 0 else (z + left) & 7

    def slot(t, way):
        return 2 * t + way if t < 3 else 6

    def send_sum(k, h, way, t):
        start(
            remote(
                pbuf.at[k, block_rows(k, h, sent_block(k, h, way, t)), :],
                rbuf.at[k, h, slot(t, way)],
                rs_send.at[k],
                rs_recv.at[k, h, t],
                (p, z_down if way == 0 else z_up),
            )
        )

    def mask_of(k, index):
        return s_in[k // 4, index].astype(F32)

    def half_copy(k):
        rows = pl.ds(pl.multiple_of(256 * (1 - far), 256), 256)
        at = across_first.index(k)
        return remote(pbuf.at[k, rows, :], xhalf.at[at], xs_send.at[k], xs_recv.at[k], (p, across))

    def st_product(k):
        came(pieces(k, 8), xg_recv.at[k, 4])
        x_high, x_low = split(xbuf[k] * mask_of(k, q))
        for m in range(4):
            at = slice(128 * m, 128 * m + 128)
            pbuf[k, at, :] = dot(a_high[at, :], x_high) + dot(a_high[at, :], x_low) + dot(a_low[at, :], x_high)
        if k in across_first:
            half_copy(k).start()

    def st_launch(k):
        if k in across_first:
            half_copy(k).wait_recv()
            rows = pl.ds(pl.multiple_of(256 * far, 256), 256)
            pbuf[k, rows, :] = pbuf[k, rows, :] + xhalf[across_first.index(k)]
        for h in halves[k]:
            for way in range(2):
                send_sum(k, h, way, 0)

    def st_sum(k, t):
        for h in halves[k]:
            came(rbuf.at[k, h, pl.ds(2 * t, 2 if t < 3 else 1)], rs_recv.at[k, h, t])
            for way in range(2):
                if t < steps(k, h, way) - 1:
                    rows = block_rows(k, h, sent_block(k, h, way, t + 1))
                    pbuf[k, rows, :] = pbuf[k, rows, :] + rbuf[k, h, slot(t, way)]
                    send_sum(k, h, way, t + 1)
        if t == 3:
            for h in halves[k]:
                total = pbuf[k, block_rows(k, h, z), :]
                for way in range(2):
                    total = total + rbuf[k, h, slot(steps(k, h, way) - 1, way)]
                sbuf[k, h] = total
            if k not in across_first:
                start(remote(sbuf.at[k, 1 - far], xrec.at[k], xs_send.at[k], xs_recv.at[k], (p, across)))

    core = p & 1
    side = (p >> 1) & 1
    mine = p & 3

    def spread_copy(t):
        return remote(e1s.at[t >> 2], e1r.at[p], e1_send.at[0], e1_recv.at[0], (t, q))

    def st_spread(k):
        def one(i, carry):
            spread_copy((p + i) & 15).start()
            return carry

        lax.fori_loop(1, GRID, one, 0)
        e1r[p] = e1s[p >> 2]

    y_rows = pl.ds(pl.multiple_of(ROWS * p, ROWS), ROWS)

    def y_copy(k, row):
        return remote(ystage.at[k], yq.at[k // 4, y_rows, :], yg_send.at[0], yg_recv.at[k // 4], (row, q))

    def st_panel(k):
        if k in across_first:
            total = sbuf[k, 0]
        else:
            came(xrec.at[k], xs_recv.at[k])
            total = sbuf[k, far] + xrec[k]
        y = total * (-mask_of(k, p))
        ystage[k] = y
        y_out[pl.ds(k, ROWS, stride=12), :] = y
        for up in (8, 4, 12, 0):
            row = 4 * (((p + up) & 15) >> 2) + k % 4
            if up:
                y_copy(k, row).start()
            else:

                @pl.when(mine != k % 4)
                def _():
                    y_copy(k, row).start()

                @pl.when(mine == k % 4)
                def _():
                    yq[k // 4, y_rows, :] = y

    def st_spread_wait(k):
        came(e1r.at[pl.ds(0, GRID - 1)], e1_recv.at[0])
        for n in range(NSUP):
            l_high[n], l_low[n] = split(e1r[:, n].reshape(WIDTH, 128).T)

    same = mine == (q >> 2)

    def e2_copy(n, w, t):
        return remote(
            e2s.at[n, w, t], e2r.at[n, q], e2_send.at[0], e2_recv.at[n], (p - mine + w, 4 * mine + t)
        )

    def st_diagonal(n):
        came(yq.at[n, pl.ds(0, ROWS * (GRID - 1)), :], yg_recv.at[n])
        y_high, y_low = split(yq[n])
        total = dot(l_high[n], y_high) + dot(l_high[n], y_low) + dot(l_low[n], y_high)
        for w in range(4):

            def put(t, tile, w=w):
                e2s[n, w, t] = tile

            pack(total[32 * w : 32 * w + 32, :], put)
        for w in range(4):
            for t in range(4):

                @pl.when(jnp.logical_or(mine != w, 4 * mine + t != q))
                def _():
                    e2_copy(n, w, t).start()

        @pl.when(same)
        def _():
            e2r[n, q] = e2s[n, mine, q & 3]

    def st_result(n):
        @pl.when(same)
        def _():
            came(e2r.at[n, pl.ds(0, GRID - 1)], e2_recv.at[n])

        @pl.when(jnp.logical_not(same))
        def _():
            came(e2r.at[n], e2_recv.at[n])

        total = jnp.sum(e2r[n], axis=0)
        parts = [total] + [pltpu.roll(total, 128 - 32 * u, 1) for u in range(1, 4)]
        square = jnp.concatenate(parts, axis=0)
        d_out[n] = piv_in[n] - square[:, :ROWS]

    def st_drain(n):
        if n == 0:

            @pl.when(jnp.logical_not(keeps))
            def _():
                went(src, a_send.at[0])

            @pl.when(jnp.logical_not(stays))
            def _():
                went(taken, land_send.at[0])

            went(xbuf.at[:, pl.ds(0, 15 * ROWS), :], xg_send.at[0])
            went(e1r.at[pl.ds(0, GRID - 1)], e1_send.at[0])
            return
        for k in range(UNITS):
            if k in across_first:
                half_copy(k).wait_send()
                went(rbuf.at[k, 0], rs_send.at[k])
            else:
                went(xrec.at[k], xs_send.at[k])
                went(rbuf.at[k], rs_send.at[k])
        went(yq.at[:, pl.ds(0, ROWS * (GRID - 1)), :], yg_send.at[0])

    stages = {
        "drain": st_drain,
        "take": st_take,
        "prepare": st_prepare,
        "own": st_own,
        "second": st_second,
        "forward": st_forward,
        "product": st_product,
        "launch": st_launch,
        "panel": st_panel,
        "spread": st_spread,
        "arrived": st_spread_wait,
        "diagonal": st_diagonal,
        "result": st_result,
    }
    for t in range(4):
        stages[f"sum{t}"] = lambda k, t=t: st_sum(k, t)
    for name, k in ORDER:
        with jax.named_scope(f"{name}_{k}"):
            stages[name](k)

    @pl.when(same)
    def _():
        went(e2r.at[:, pl.ds(0, GRID - 1)], e2_send.at[0])

    @pl.when(jnp.logical_not(same))
    def _():
        went(e2r, e2_send.at[0])


def body(ancestor_inverse, factor_panel, pivot_inverse, structure):
    hbm = pl.BlockSpec(memory_space=pltpu.HBM)
    dma = pltpu.SemaphoreType.DMA
    panel, diagonal = pl.pallas_call(
        kernel,
        out_shape=(
            pltpu.VMEM((ROWS * NSUP * 4, 128), F32),
            pltpu.VMEM(pivot_inverse.shape, F32),
        ),
        in_specs=[hbm] * 4,
        out_specs=(pl.BlockSpec(memory_space=pltpu.VMEM),)*2,
        scratch_shapes=[
            pltpu.VMEM((WIDTH, WIDTH), F32),
            pltpu.VMEM((ROWS * NSUP * 4, 128), F32),
            pltpu.VMEM((NSUP, ROWS, ROWS), F32),
            pltpu.SMEM((NSUP, GRID), jnp.int32),
            pltpu.VMEM((WIDTH, WIDTH), BF16),
            pltpu.VMEM((WIDTH, WIDTH), BF16),
            pltpu.VMEM((UNITS, ROWS, COLS), F32),
            pltpu.VMEM((UNITS, ROWS, COLS), F32),
            pltpu.VMEM((UNITS, WIDTH, COLS), F32),
            pltpu.VMEM((UNITS, WIDTH, COLS), F32),
            pltpu.VMEM((UNITS, 2, 7, ROWS, COLS), F32),
            pltpu.VMEM((UNITS, 2, ROWS, COLS), F32),
            pltpu.VMEM((UNITS, ROWS, COLS), F32),
            pltpu.VMEM((len(FIRST_ACROSS), 256, COLS), F32),
            pltpu.VMEM((UNITS, ROWS, COLS), F32),
            pltpu.VMEM((NSUP, WIDTH, 128), F32),
            pltpu.VMEM((NSUP, 128, WIDTH), BF16),
            pltpu.VMEM((NSUP, 128, WIDTH), BF16),
            pltpu.VMEM((4, NSUP, ROWS, 128), F32),
            pltpu.VMEM((GRID, NSUP, ROWS, 128), F32),
            pltpu.VMEM((NSUP, 4, 4, 8, 128), F32),
            pltpu.VMEM((NSUP, GRID, 8, 128), F32),
            dma((4,)),
            dma((1,)),
            dma((UNITS,)),
            dma((1,)),
            dma((1,)),
            dma((UNITS, 5)),
            dma((UNITS,)),
            dma((UNITS, 2, 4)),
            dma((UNITS,)),
            dma((UNITS,)),
            dma((1,)),
            dma((NSUP,)),
            dma((1,)),
            dma((1,)),
            dma((1,)),
            dma((NSUP,)),
        ],
        compiler_params=pltpu.CompilerParams(
            collective_id=0, has_side_effects=True, vmem_limit_bytes=VMEM_LIMIT
        ),
        name="level",
    )(
        pltpu.with_memory_space_constraint(ancestor_inverse.reshape(WIDTH, WIDTH), pltpu.HBM),
        pltpu.with_memory_space_constraint(factor_panel.reshape(ROWS * NSUP * 4, 128), pltpu.HBM),
        pltpu.with_memory_space_constraint(pivot_inverse, pltpu.HBM),
        pltpu.with_memory_space_constraint(structure.T, pltpu.HBM),
    )
    return panel.reshape(ROWS, 1, NSUP, WIDTH), diagonal


def solution(mesh):
    return jax.shard_map(
        body,
        mesh=mesh,
        in_specs=(
            P("prow", "pcol", None, None),
            P("pcol", "prow", None, None),
            P(None, "prow", "pcol"),
            P(),
        ),
        out_specs=(P("pcol", "prow", None, None), P(None, "prow", "pcol")),
        check_vma=False,
    )
```

```python
import jax
import jax.numpy as jnp
from jax import lax
from jax.experimental import pallas as pl
from jax.experimental.pallas import tpu as pltpu
from jax.sharding import PartitionSpec as P

F32 = jnp.float32
BF16 = jnp.bfloat16
MESH = pl.DeviceIdType.MESH
ROWS = 32
NSUP = 3
WIDTH = 512
GRID = 16
UNITS = 12
COLS = 128
IN_FLIGHT = 3
FIRST_ACROSS = (2, 4, 7, 9)


VMEM_LIMIT = 40 * 1024 * 1024


ORDER = (
    ("take", 0), ("prepare", 0), ("take", 1), ("take", 2), ("take", 3), ("take", 4), ("take", 5), ("take", 6),
    ("take", 7), ("take", 8), ("take", 9), ("take", 10), ("take", 11), ("own", 0), ("second", 0), ("own", 1),
    ("second", 1), ("own", 2), ("second", 2), ("own", 3), ("second", 3), ("own", 4), ("second", 4),
    ("own", 5), ("forward", 0), ("second", 5), ("own", 6), ("second", 6), ("own", 7), ("forward", 1),
    ("product", 0), ("second", 7), ("own", 8), ("launch", 0), ("second", 8), ("own", 9), ("forward", 2),
    ("product", 1), ("second", 9), ("own", 10), ("launch", 1), ("second", 10), ("own", 11), ("forward", 3),
    ("product", 2), ("sum0", 0), ("second", 11), ("forward", 4), ("product", 3), ("sum0", 1), ("launch", 3),
    ("forward", 5), ("product", 4), ("sum1", 0), ("forward", 6), ("product", 5), ("sum1", 1), ("launch", 5),
    ("sum0", 3), ("forward", 7), ("product", 6), ("sum2", 0), ("launch", 6), ("launch", 2), ("forward", 8),
    ("product", 7), ("sum2", 1), ("sum0", 5), ("forward", 9), ("product", 8), ("sum1", 3), ("launch", 8),
    ("launch", 4), ("sum3", 0), ("forward", 10), ("sum0", 6), ("product", 9), ("sum0", 2), ("sum3", 1),
    ("forward", 11), ("sum1", 5), ("product", 10), ("launch", 10), ("sum2", 3), ("sum0", 8), ("product", 11),
    ("sum0", 4), ("launch", 11), ("spread", 0), ("panel", 0), ("sum1", 6), ("sum1", 2), ("sum2", 5),
    ("sum0", 10), ("sum3", 3), ("launch", 7), ("sum1", 8), ("panel", 1), ("sum1", 4), ("sum0", 11),
    ("sum2", 6), ("sum2", 2), ("sum3", 5), ("launch", 9), ("sum1", 10), ("sum0", 7), ("sum2", 8), ("sum2", 4),
    ("sum1", 11), ("sum3", 6), ("sum3", 2), ("panel", 2), ("sum0", 9), ("sum2", 10), ("sum1", 7), ("sum3", 8),
    ("sum3", 4), ("panel", 4), ("sum2", 11), ("sum1", 9), ("sum3", 10), ("panel", 3), ("sum2", 7),
    ("panel", 5), ("sum3", 11), ("panel", 6), ("sum2", 9), ("sum3", 7), ("panel", 8), ("panel", 7),
    ("panel", 10), ("sum3", 9), ("panel", 9), ("arrived", 0), ("diagonal", 0), ("panel", 11), ("drain", 0),
    ("diagonal", 1), ("diagonal", 2), ("drain", 1), ("result", 0), ("result", 1), ("result", 2),
)


def split(x):
    high = x.astype(BF16)
    return high, (x - high.astype(F32)).astype(BF16)


def dot(a, b):
    return jnp.dot(a, b, preferred_element_type=F32)


def passing(row, chunk):
    bit = chunk & 1
    turn = 2 * (((row >> 1) ^ (chunk >> 1)) & 1) + (((chunk >> 2) & 1) ^ bit)
    return row ^ (4 * turn + bit)


def landing(row, block, chunk):
    return row ^ (2 * (((block >> 3) ^ (chunk >> 3)) & 1))


def chunk_at(row, block):
    high = ((row >> 1) ^ (block >> 1)) & 1
    low = row & 1
    middle = ((row >> 3) ^ (block >> 3)) & 1
    third = ((row >> 2) ^ block ^ low) & 1
    return block ^ (8 * high + 4 * third + 2 * middle + low)


def pack(y, put):
    lane = lax.broadcasted_iota(jnp.int32, (8, 128), 1) >> 5
    for g in range(y.shape[1] // 128):
        tiles = [y[8 * u : 8 * u + 8, 128 * g : 128 * g + 128] for u in range(4)]
        for h in range(4):
            out = None
            for u in range(4):
                by = (32 * (u - h)) % 128
                moved = pltpu.roll(tiles[u], by, 1) if by else tiles[u]
                out = moved if out is None else jnp.where(lane == u, moved, out)
            put(4 * g + h, out)


def kernel(
    a_hbm, l_hbm, piv_hbm, s_hbm,
    y_out, d_out,
    a_in, l_in, piv_in, s_in, a_high, a_low, src, taken, xbuf, pbuf, rbuf, sbuf, xrec, xhalf, ystage, yq, l_high, l_low,
    e1s, e1r, e2s, e2r,
    load_sem, a_send, a_recv, land_send, xg_send, xg_recv, rs_send, rs_recv, xs_send, xs_recv, yg_send, yg_recv,
    e1_send, e1_recv, e2_send, e2_recv,
):
    p = lax.axis_index("prow")
    q = lax.axis_index("pcol")
    z = q & 7
    far = q >> 3

    loads = [
        pltpu.make_async_copy(source, target, load_sem.at[n])
        for n, (source, target) in enumerate(((l_hbm, l_in), (a_hbm, a_in), (s_hbm, s_in), (piv_hbm, piv_in)))
    ]
    for load in loads:
        load.start()

    other = p ^ 1
    beside = p ^ 2
    above = (p + 4) & 15
    below = (p - 4) & 15
    z_up = (q & 8) + ((z + 1) & 7)
    z_down = (q & 8) + ((z - 1) & 7)
    across = q ^ 8

    taker = passing(p, q)
    keeps = taker == p
    block = taker
    target_row = landing(p, block, q)
    stays = block == q
    origin = chunk_at(p, q)
    origin_row = landing(p, q, origin)
    second = chunk_at(beside, q)
    second_row = landing(beside, q, second)

    barrier = pltpu.get_barrier_semaphore()
    opposite = (p + 8) & 15
    for device in (
        (other, q), (beside, q), (above, q), (below, q), (opposite, q), (p, z_up), (p, z_down), (p, across)
    ):
        pl.semaphore_signal(barrier, inc=1, device_id=device, device_id_type=MESH)

    @pl.when(jnp.logical_not(keeps))
    def _():
        pl.semaphore_signal(barrier, inc=1, device_id=(taker, q), device_id_type=MESH)

    @pl.when(jnp.logical_not(stays))
    def _():
        pl.semaphore_signal(barrier, inc=1, device_id=(target_row, block), device_id_type=MESH)

    @pl.when(origin != q)
    def _():
        pl.semaphore_signal(barrier, inc=1, device_id=(origin_row, origin), device_id_type=MESH)

    pl.semaphore_signal(barrier, inc=1, device_id=(target_row ^ 2, block), device_id_type=MESH)
    pl.semaphore_signal(barrier, inc=1, device_id=(second_row, second), device_id_type=MESH)

    loads[0].wait()
    for u in range(UNITS):
        src[u] = l_in[pl.ds(u, ROWS, stride=12), :]
    with jax.named_scope("barrier"):
        pl.semaphore_wait(
            barrier, jnp.where(keeps, 10, 11) + jnp.where(stays, 0, 1) + jnp.where(origin == q, 0, 1)
        )

    def start(copy):
        copy.start()

    def came(ref, sem):
        remote(ref, ref, sem, sem, (other, q)).wait_recv()

    def went(ref, sem):
        remote(ref, ref, sem, sem, (other, q)).wait_send()

    def remote(source, target, send, recv, device):
        return pltpu.make_async_remote_copy(
            src_ref=source, dst_ref=target, send_sem=send, recv_sem=recv, device_id=device, device_id_type=MESH
        )

    kinds = (p, beside, below, below ^ 2, above, above ^ 2, opposite, opposite ^ 2)
    kinds = kinds + tuple(kind ^ 1 for kind in kinds)

    where = [pl.ds(pl.multiple_of(ROWS * chunk_at(kind, q), ROWS), ROWS) for kind in kinds]

    def piece(k, kind):
        return xbuf.at[k, where[kind], :]

    def push(k, kind, as_kind, row):
        group = as_kind if as_kind < 2 else 2 if as_kind < 6 else 3 if as_kind < 8 else 4
        start(remote(piece(k, kind), piece(k, kind), xg_send.at[0], xg_recv.at[k, group], (row, q)))

    def pieces(k, count):
        return xbuf.at[k, pl.ds(0, ROWS * count), :]

    def push_all(k, kind):
        push(k, kind, 6 + kind, opposite)
        push(k, kind, 2 + kind, above)
        push(k, kind, 4 + kind, below)
        push(k, kind, 8 + kind, other)

    def take_copy(k):
        return remote(src.at[k], taken.at[k], a_send.at[0], a_recv.at[k], (taker, q))

    def land_copy(k, aside):
        rows = pl.ds(pl.multiple_of(ROWS * q, ROWS), ROWS)
        return remote(
            taken.at[k],
            xbuf.at[k, rows, :],
            land_send.at[0] if aside == 0 else xg_send.at[0],
            xg_recv.at[k, aside],
            (target_row ^ (2 * aside), block),
        )

    for k in range(UNITS):

        @pl.when(jnp.logical_not(keeps))
        def _():
            take_copy(k).start()

        @pl.when(keeps)
        def _():
            taken[k] = src[k]

    def st_take(k):
        @pl.when(jnp.logical_not(keeps))
        def _():
            take_copy(k).wait_recv()

        @pl.when(jnp.logical_not(stays))
        def _():
            land_copy(k, 0).start()

        land_copy(k, 1).start()

        @pl.when(stays)
        def _():
            xbuf[k, where[0], :] = taken[k]

    def st_prepare(k):
        loads[1].wait()
        a_high[...], a_low[...] = split(a_in[...])
        for n in range(NSUP):
            for g in range(4):
                e1s[g, n] = src[4 * n + g]
        loads[2].wait()
        loads[3].wait()

    def st_own(k):
        @pl.when(origin != q)
        def _():
            came(pieces(k, 1), xg_recv.at[k, 0])

        push_all(k, 0)

    def st_second(k):
        came(pieces(k, 1), xg_recv.at[k, 1])
        push_all(k, 1)

    def st_forward(k):
        came(pieces(k, 4), xg_recv.at[k, 2])
        for kind in range(2, 6):
            push(k, kind, 8 + kind, other)
        came(pieces(k, 2), xg_recv.at[k, 3])
        for kind in range(6, 8):
            push(k, kind, 8 + kind, other)

    across_first = FIRST_ACROSS
    halves = [(0,) if k in across_first else (0, 1) for k in range(UNITS)]

    flows = [(k, h) for k in range(UNITS) for h in halves[k]]

    def steps(k, h, way):
        return 4 if (k + h + way) % 2 == 0 else 3

    def block_rows(k, h, d):
        half = far if k in across_first else h
        return pl.ds(pl.multiple_of(256 * half + ROWS * d, ROWS), ROWS)

    def sent_block(k, h, way, t):
        left = steps(k, h, way) - t
        return (z - left) & 7 if way == 0 else (z + left) & 7

    def slot(t, way):
        return 2 * t + way if t < 3 else 6

    def send_sum(k, h, way, t):
        start(
            remote(
                pbuf.at[k, block_rows(k, h, sent_block(k, h, way, t)), :],
                rbuf.at[k, h, slot(t, way)],
                rs_send.at[0],
                rs_recv.at[flows.index((k, h)), t],
                (p, z_down if way == 0 else z_up),
            )
        )

    def mask_of(k, index):
        return s_in[k // 4, index].astype(F32)

    def half_copy(k):
        rows = pl.ds(pl.multiple_of(256 * (1 - far), 256), 256)
        at = across_first.index(k)
        return remote(pbuf.at[k, rows, :], xhalf.at[at], xs_send.at[0], xs_recv.at[k], (p, across))

    def st_product(k):
        came(pieces(k, 8), xg_recv.at[k, 4])
        x_high, x_low = split(xbuf[k] * mask_of(k, q))
        for m in range(4):
            at = slice(128 * m, 128 * m + 128)
            pbuf[k, at, :] = dot(a_high[at, :], x_high) + dot(a_high[at, :], x_low) + dot(a_low[at, :], x_high)
        if k in across_first:
            half_copy(k).start()

    def st_launch(k):
        if k in across_first:
            half_copy(k).wait_recv()
            rows = pl.ds(pl.multiple_of(256 * far, 256), 256)
            pbuf[k, rows, :] = pbuf[k, rows, :] + xhalf[across_first.index(k)]
        for h in halves[k]:
            for way in range(2):
                send_sum(k, h, way, 0)

    def st_sum(k, t):
        for h in halves[k]:
            came(rbuf.at[k, h, pl.ds(2 * t, 2 if t < 3 else 1)], rs_recv.at[flows.index((k, h)), t])
            for way in range(2):
                if t < steps(k, h, way) - 1:
                    rows = block_rows(k, h, sent_block(k, h, way, t + 1))
                    pbuf[k, rows, :] = pbuf[k, rows, :] + rbuf[k, h, slot(t, way)]
                    send_sum(k, h, way, t + 1)
        if t == 3:
            for h in halves[k]:
                total = pbuf[k, block_rows(k, h, z), :]
                for way in range(2):
                    total = total + rbuf[k, h, slot(steps(k, h, way) - 1, way)]
                sbuf[k, h] = total
            if k not in across_first:
                start(remote(sbuf.at[k, 1 - far], xrec.at[k], xs_send.at[0], xs_recv.at[k], (p, across)))

    core = p & 1
    side = (p >> 1) & 1
    mine = p & 3

    def spread_copy(t):
        return remote(e1s.at[t >> 2], e1r.at[p], e1_send.at[0], e1_recv.at[0], (t, q))

    def st_spread(k):
        def one(i, carry):
            spread_copy((p + i) & 15).start()
            return carry

        lax.fori_loop(1, GRID, one, 0)
        e1r[p] = e1s[p >> 2]

    y_rows = pl.ds(pl.multiple_of(ROWS * p, ROWS), ROWS)

    def y_copy(k, row):
        return remote(ystage.at[k], yq.at[k // 4, y_rows, :], yg_send.at[0], yg_recv.at[k // 4], (row, q))

    def st_panel(k):
        if k in across_first:
            total = sbuf[k, 0]
        else:
            came(xrec.at[k], xs_recv.at[k])
            total = sbuf[k, far] + xrec[k]
        y = total * (-mask_of(k, p))
        ystage[k] = y
        y_out[pl.ds(k, ROWS, stride=12), :] = y
        for up in (8, 4, 12, 0):
            row = 4 * (((p + up) & 15) >> 2) + k % 4
            if up:
                y_copy(k, row).start()
            else:

                @pl.when(mine != k % 4)
                def _():
                    y_copy(k, row).start()

                @pl.when(mine == k % 4)
                def _():
                    yq[k // 4, y_rows, :] = y

    def st_spread_wait(k):
        came(e1r.at[pl.ds(0, GRID - 1)], e1_recv.at[0])
        for n in range(NSUP):
            l_high[n], l_low[n] = split(e1r[:, n].reshape(WIDTH, 128).T)

    same = mine == (q >> 2)

    def e2_copy(n, w, t):
        return remote(
            e2s.at[n, w, t], e2r.at[n, q], e2_send.at[0], e2_recv.at[n], (p - mine + w, 4 * mine + t)
        )

    def st_diagonal(n):
        came(yq.at[n, pl.ds(0, ROWS * (GRID - 1)), :], yg_recv.at[n])
        y_high, y_low = split(yq[n])
        total = dot(l_high[n], y_high) + dot(l_high[n], y_low) + dot(l_low[n], y_high)
        for w in range(4):

            def put(t, tile, w=w):
                e2s[n, w, t] = tile

            pack(total[32 * w : 32 * w + 32, :], put)
        for w in range(4):
            for t in range(4):

                @pl.when(jnp.logical_or(mine != w, 4 * mine + t != q))
                def _():
                    e2_copy(n, w, t).start()

        @pl.when(same)
        def _():
            e2r[n, q] = e2s[n, mine, q & 3]

    def st_result(n):
        @pl.when(same)
        def _():
            came(e2r.at[n, pl.ds(0, GRID - 1)], e2_recv.at[n])

        @pl.when(jnp.logical_not(same))
        def _():
            came(e2r.at[n], e2_recv.at[n])

        total = jnp.sum(e2r[n], axis=0)
        parts = [total] + [pltpu.roll(total, 128 - 32 * u, 1) for u in range(1, 4)]
        square = jnp.concatenate(parts, axis=0)
        d_out[n] = piv_in[n] - square[:, :ROWS]

    def st_drain(n):
        if n == 0:

            @pl.when(jnp.logical_not(keeps))
            def _():
                went(src, a_send.at[0])

            @pl.when(jnp.logical_not(stays))
            def _():
                went(taken, land_send.at[0])

            went(xbuf.at[:, pl.ds(0, 15 * ROWS), :], xg_send.at[0])
            went(e1r.at[pl.ds(0, GRID - 1)], e1_send.at[0])
            return
        went(xbuf.at[pl.ds(0, 5), pl.ds(0, 256), :], xs_send.at[0])
        went(rbuf.at[pl.ds(0, UNITS - len(across_first) // 2)], rs_send.at[0])
        went(yq.at[:, pl.ds(0, ROWS * (GRID - 1)), :], yg_send.at[0])

    stages = {
        "drain": st_drain,
        "take": st_take,
        "prepare": st_prepare,
        "own": st_own,
        "second": st_second,
        "forward": st_forward,
        "product": st_product,
        "launch": st_launch,
        "panel": st_panel,
        "spread": st_spread,
        "arrived": st_spread_wait,
        "diagonal": st_diagonal,
        "result": st_result,
    }
    for t in range(4):
        stages[f"sum{t}"] = lambda k, t=t: st_sum(k, t)
    for name, k in ORDER:
        with jax.named_scope(f"{name}_{k}"):
            stages[name](k)

    @pl.when(same)
    def _():
        went(e2r.at[:, pl.ds(0, GRID - 1)], e2_send.at[0])

    @pl.when(jnp.logical_not(same))
    def _():
        went(e2r, e2_send.at[0])


def body(ancestor_inverse, factor_panel, pivot_inverse, structure):
    hbm = pl.BlockSpec(memory_space=pltpu.HBM)
    dma = pltpu.SemaphoreType.DMA
    panel, diagonal = pl.pallas_call(
        kernel,
        out_shape=(
            pltpu.VMEM((ROWS * NSUP * 4, 128), F32),
            pltpu.VMEM(pivot_inverse.shape, F32),
        ),
        in_specs=[hbm] * 4,
        out_specs=(pl.BlockSpec(memory_space=pltpu.VMEM),)*2,
        scratch_shapes=[
            pltpu.VMEM((WIDTH, WIDTH), F32),
            pltpu.VMEM((ROWS * NSUP * 4, 128), F32),
            pltpu.VMEM((NSUP, ROWS, ROWS), F32),
            pltpu.SMEM((NSUP, GRID), jnp.int32),
            pltpu.VMEM((WIDTH, WIDTH), BF16),
            pltpu.VMEM((WIDTH, WIDTH), BF16),
            pltpu.VMEM((UNITS, ROWS, COLS), F32),
            pltpu.VMEM((UNITS, ROWS, COLS), F32),
            pltpu.VMEM((UNITS, WIDTH, COLS), F32),
            pltpu.VMEM((UNITS, WIDTH, COLS), F32),
            pltpu.VMEM((UNITS, 2, 7, ROWS, COLS), F32),
            pltpu.VMEM((UNITS, 2, ROWS, COLS), F32),
            pltpu.VMEM((UNITS, ROWS, COLS), F32),
            pltpu.VMEM((len(FIRST_ACROSS), 256, COLS), F32),
            pltpu.VMEM((UNITS, ROWS, COLS), F32),
            pltpu.VMEM((NSUP, WIDTH, 128), F32),
            pltpu.VMEM((NSUP, 128, WIDTH), BF16),
            pltpu.VMEM((NSUP, 128, WIDTH), BF16),
            pltpu.VMEM((4, NSUP, ROWS, 128), F32),
            pltpu.VMEM((GRID, NSUP, ROWS, 128), F32),
            pltpu.VMEM((NSUP, 4, 4, 8, 128), F32),
            pltpu.VMEM((NSUP, GRID, 8, 128), F32),
            dma((4,)),
            dma((1,)),
            dma((UNITS,)),
            dma((1,)),
            dma((1,)),
            dma((UNITS, 5)),
            dma((1,)),
            dma((2 * UNITS - len(FIRST_ACROSS), 4)),
            dma((1,)),
            dma((UNITS,)),
            dma((1,)),
            dma((NSUP,)),
            dma((1,)),
            dma((1,)),
            dma((1,)),
            dma((NSUP,)),
        ],
        compiler_params=pltpu.CompilerParams(
            collective_id=0, has_side_effects=True, vmem_limit_bytes=VMEM_LIMIT
        ),
        name="level",
    )(
        pltpu.with_memory_space_constraint(ancestor_inverse.reshape(WIDTH, WIDTH), pltpu.HBM),
        pltpu.with_memory_space_constraint(factor_panel.reshape(ROWS * NSUP * 4, 128), pltpu.HBM),
        pltpu.with_memory_space_constraint(pivot_inverse, pltpu.HBM),
        pltpu.with_memory_space_constraint(structure.T, pltpu.HBM),
    )
    return panel.reshape(ROWS, 1, NSUP, WIDTH), diagonal


def solution(mesh):
    return jax.shard_map(
        body,
        mesh=mesh,
        in_specs=(
            P("prow", "pcol", None, None),
            P("pcol", "prow", None, None),
            P(None, "prow", "pcol"),
            P(),
        ),
        out_specs=(P("pcol", "prow", None, None), P(None, "prow", "pcol")),
        check_vma=False,
    )
```

```python
import jax
import jax.numpy as jnp
from jax import lax
from jax.experimental import pallas as pl
from jax.experimental.pallas import tpu as pltpu
from jax.sharding import PartitionSpec as P

F32 = jnp.float32
BF16 = jnp.bfloat16
MESH = pl.DeviceIdType.MESH
ROWS = 32
NSUP = 3
WIDTH = 512
GRID = 16
UNITS = 12
COLS = 128
IN_FLIGHT = 3
FIRST_ACROSS = (2, 4, 7, 9)


VMEM_LIMIT = 40 * 1024 * 1024


ORDER = (
    ("take", 0), ("prepare", 0), ("take", 1), ("take", 2), ("take", 3), ("take", 4), ("take", 5), ("take", 6),
    ("take", 7), ("take", 8), ("take", 9), ("take", 10), ("take", 11), ("own", 0), ("second", 0), ("own", 1),
    ("second", 1), ("own", 2), ("second", 2), ("own", 3), ("second", 3), ("own", 4), ("second", 4),
    ("own", 5), ("forward", 0), ("second", 5), ("own", 6), ("second", 6), ("own", 7), ("forward", 1),
    ("product", 0), ("second", 7), ("own", 8), ("launch", 0), ("second", 8), ("own", 9), ("forward", 2),
    ("product", 1), ("second", 9), ("own", 10), ("launch", 1), ("second", 10), ("own", 11), ("forward", 3),
    ("product", 2), ("sum0", 0), ("second", 11), ("forward", 4), ("product", 3), ("sum0", 1), ("launch", 3),
    ("forward", 5), ("product", 4), ("sum1", 0), ("forward", 6), ("product", 5), ("sum1", 1), ("launch", 5),
    ("sum0", 3), ("forward", 7), ("product", 6), ("sum2", 0), ("launch", 2), ("launch", 6), ("forward", 8),
    ("product", 7), ("sum2", 1), ("sum0", 5), ("forward", 9), ("product", 8), ("sum1", 3), ("launch", 4),
    ("launch", 8), ("sum3", 0), ("sum0", 2), ("forward", 10), ("product", 9), ("sum0", 6), ("spread", 0),
    ("sum3", 1), ("forward", 11), ("sum1", 5), ("product", 10), ("launch", 10), ("sum2", 3), ("sum0", 4),
    ("product", 11), ("sum0", 8), ("launch", 7), ("panel", 0), ("sum1", 2), ("sum1", 6), ("sum2", 5),
    ("sum0", 10), ("sum3", 3), ("launch", 11), ("sum1", 4), ("sum1", 8), ("sum0", 7), ("sum2", 2),
    ("sum2", 6), ("sum3", 5), ("launch", 9), ("sum1", 10), ("sum0", 11), ("sum2", 4), ("sum2", 8),
    ("sum1", 7), ("sum3", 2), ("panel", 2), ("sum3", 6), ("sum0", 9), ("sum2", 10), ("sum1", 11), ("sum3", 4),
    ("panel", 4), ("sum3", 8), ("panel", 1), ("sum2", 7), ("sum1", 9), ("sum3", 10), ("panel", 3),
    ("panel", 5), ("sum2", 11), ("sum3", 7), ("panel", 7), ("panel", 6), ("sum2", 9), ("panel", 8),
    ("sum3", 11), ("panel", 10), ("sum3", 9), ("panel", 9), ("arrived", 0), ("diagonal", 0), ("diagonal", 1),
    ("panel", 11), ("drain", 0), ("diagonal", 2), ("drain", 1), ("result", 0), ("result", 1), ("result", 2),
)


def split(x):
    high = x.astype(BF16)
    return high, (x - high.astype(F32)).astype(BF16)


def dot(a, b):
    return jnp.dot(a, b, preferred_element_type=F32)


def passing(row, chunk):
    bit = chunk & 1
    turn = 2 * (((row >> 1) ^ (chunk >> 1)) & 1) + (((chunk >> 2) & 1) ^ bit)
    return row ^ (4 * turn + bit)


def landing(row, block, chunk):
    return row ^ (2 * (((block >> 3) ^ (chunk >> 3)) & 1))


def chunk_at(row, block):
    high = ((row >> 1) ^ (block >> 1)) & 1
    low = row & 1
    middle = ((row >> 3) ^ (block >> 3)) & 1
    third = ((row >> 2) ^ block ^ low) & 1
    return block ^ (8 * high + 4 * third + 2 * middle + low)


def pack(y, put):
    lane = lax.broadcasted_iota(jnp.int32, (8, 128), 1) >> 5
    for g in range(y.shape[1] // 128):
        tiles = [y[8 * u : 8 * u + 8, 128 * g : 128 * g + 128] for u in range(4)]
        for h in range(4):
            out = None
            for u in range(4):
                by = (32 * (u - h)) % 128
                moved = pltpu.roll(tiles[u], by, 1) if by else tiles[u]
                out = moved if out is None else jnp.where(lane == u, moved, out)
            put(4 * g + h, out)


def kernel(
    a_hbm, l_hbm, piv_hbm, s_hbm,
    y_out, d_out,
    a_in, l_in, piv_in, s_in, a_high, a_low, src, taken, xbuf, pbuf, rbuf, sbuf, xrec, xhalf, ystage, yq, l_high, l_low,
    e1s, e1r, e2s, e2r,
    load_sem, a_send, a_recv, land_send, xg_send, xg_recv, rs_send, rs_recv, xs_send, xs_recv, yg_send, yg_recv,
    e1_send, e1_recv, e2_send, e2_recv,
):
    p = lax.axis_index("prow")
    q = lax.axis_index("pcol")
    z = q & 7
    far = q >> 3

    loads = [
        pltpu.make_async_copy(source, target, load_sem.at[n])
        for n, (source, target) in enumerate(((l_hbm, l_in), (a_hbm, a_in), (s_hbm, s_in), (piv_hbm, piv_in)))
    ]
    for load in loads:
        load.start()

    other = p ^ 1
    beside = p ^ 2
    above = (p + 4) & 15
    below = (p - 4) & 15
    z_up = (q & 8) + ((z + 1) & 7)
    z_down = (q & 8) + ((z - 1) & 7)
    across = q ^ 8

    taker = passing(p, q)
    keeps = taker == p
    block = taker
    target_row = landing(p, block, q)
    stays = block == q
    origin = chunk_at(p, q)
    origin_row = landing(p, q, origin)
    second = chunk_at(beside, q)
    second_row = landing(beside, q, second)

    barrier = pltpu.get_barrier_semaphore()
    opposite = (p + 8) & 15
    for device in (
        (other, q), (beside, q), (above, q), (below, q), (opposite, q), (p, z_up), (p, z_down), (p, across)
    ):
        pl.semaphore_signal(barrier, inc=1, device_id=device, device_id_type=MESH)

    @pl.when(jnp.logical_not(keeps))
    def _():
        pl.semaphore_signal(barrier, inc=1, device_id=(taker, q), device_id_type=MESH)

    @pl.when(jnp.logical_not(stays))
    def _():
        pl.semaphore_signal(barrier, inc=1, device_id=(target_row, block), device_id_type=MESH)

    @pl.when(origin != q)
    def _():
        pl.semaphore_signal(barrier, inc=1, device_id=(origin_row, origin), device_id_type=MESH)

    pl.semaphore_signal(barrier, inc=1, device_id=(target_row ^ 2, block), device_id_type=MESH)
    pl.semaphore_signal(barrier, inc=1, device_id=(second_row, second), device_id_type=MESH)

    loads[0].wait()
    for u in range(UNITS):
        src[u] = l_in[pl.ds(u, ROWS, stride=12), :]
    with jax.named_scope("barrier"):
        pl.semaphore_wait(
            barrier, jnp.where(keeps, 10, 11) + jnp.where(stays, 0, 1) + jnp.where(origin == q, 0, 1)
        )

    def start(copy):
        copy.start()

    def came(ref, sem):
        remote(ref, ref, sem, sem, (other, q)).wait_recv()

    def went(ref, sem):
        remote(ref, ref, sem, sem, (other, q)).wait_send()

    def remote(source, target, send, recv, device):
        return pltpu.make_async_remote_copy(
            src_ref=source, dst_ref=target, send_sem=send, recv_sem=recv, device_id=device, device_id_type=MESH
        )

    kinds = (p, beside, below, below ^ 2, above, above ^ 2, opposite, opposite ^ 2)
    kinds = kinds + tuple(kind ^ 1 for kind in kinds)

    where = [pl.ds(pl.multiple_of(ROWS * chunk_at(kind, q), ROWS), ROWS) for kind in kinds]

    def piece(k, kind):
        return xbuf.at[k, where[kind], :]

    def push(k, kind, as_kind, row):
        group = as_kind if as_kind < 2 else 2 if as_kind < 6 else 3 if as_kind < 8 else 4
        start(remote(piece(k, kind), piece(k, kind), xg_send.at[0], xg_recv.at[k, group], (row, q)))

    def pieces(k, count):
        return xbuf.at[k, pl.ds(0, ROWS * count), :]

    def push_all(k, kind):
        push(k, kind, 6 + kind, opposite)
        push(k, kind, 2 + kind, above)
        push(k, kind, 4 + kind, below)
        push(k, kind, 8 + kind, other)

    def take_copy(k):
        return remote(src.at[k], taken.at[k], a_send.at[0], a_recv.at[k], (taker, q))

    def land_copy(k, aside):
        rows = pl.ds(pl.multiple_of(ROWS * q, ROWS), ROWS)
        return remote(
            taken.at[k],
            xbuf.at[k, rows, :],
            land_send.at[0] if aside == 0 else xg_send.at[0],
            xg_recv.at[k, aside],
            (target_row ^ (2 * aside), block),
        )

    for k in range(UNITS):

        @pl.when(jnp.logical_not(keeps))
        def _():
            take_copy(k).start()

        @pl.when(keeps)
        def _():
            taken[k] = src[k]

    def st_take(k):
        @pl.when(jnp.logical_not(keeps))
        def _():
            take_copy(k).wait_recv()

        @pl.when(jnp.logical_not(stays))
        def _():
            land_copy(k, 0).start()

        land_copy(k, 1).start()

        @pl.when(stays)
        def _():
            xbuf[k, where[0], :] = taken[k]

    def st_prepare(k):
        loads[1].wait()
        a_high[...], a_low[...] = split(a_in[...])
        for n in range(NSUP):
            for g in range(4):
                e1s[g, n] = src[4 * n + g]
        loads[2].wait()
        loads[3].wait()

    def st_own(k):
        @pl.when(origin != q)
        def _():
            came(pieces(k, 1), xg_recv.at[k, 0])

        push_all(k, 0)

    def st_second(k):
        came(pieces(k, 1), xg_recv.at[k, 1])
        push_all(k, 1)

    def st_forward(k):
        came(pieces(k, 4), xg_recv.at[k, 2])
        for kind in range(2, 6):
            push(k, kind, 8 + kind, other)
        came(pieces(k, 2), xg_recv.at[k, 3])
        for kind in range(6, 8):
            push(k, kind, 8 + kind, other)

    across_first = FIRST_ACROSS
    halves = [(0,) if k in across_first else (0, 1) for k in range(UNITS)]

    flows = [(k, h) for k in range(UNITS) for h in halves[k]]

    def steps(k, h, way):
        return 4 if (k + h + way) % 2 == 0 else 3

    def block_rows(k, h, d):
        half = far if k in across_first else h
        return pl.ds(pl.multiple_of(256 * half + ROWS * d, ROWS), ROWS)

    def sent_block(k, h, way, t):
        left = steps(k, h, way) - t
        return (z - left) & 7 if way == 0 else (z + left) & 7

    def slot(t, way):
        return 2 * t + way if t < 3 else 6

    def send_sum(k, h, way, t):
        start(
            remote(
                pbuf.at[k, block_rows(k, h, sent_block(k, h, way, t)), :],
                rbuf.at[k, h, slot(t, way)],
                rs_send.at[0],
                rs_recv.at[flows.index((k, h)), t],
                (p, z_down if way == 0 else z_up),
            )
        )

    def mask_of(k, index):
        return s_in[k // 4, index].astype(F32)

    def half_copy(k):
        rows = pl.ds(pl.multiple_of(256 * (1 - far), 256), 256)
        at = across_first.index(k)
        return remote(pbuf.at[k, rows, :], xhalf.at[at], xs_send.at[0], xs_recv.at[k], (p, across))

    def st_product(k):
        came(pieces(k, 8), xg_recv.at[k, 4])
        x_high, x_low = split(xbuf[k] * mask_of(k, q))
        for m in range(4):
            at = slice(128 * m, 128 * m + 128)
            pbuf[k, at, :] = dot(a_high[at, :], x_high) + dot(a_high[at, :], x_low) + dot(a_low[at, :], x_high)
        if k in across_first:
            half_copy(k).start()

    def st_launch(k):
        if k in across_first:
            half_copy(k).wait_recv()
            rows = pl.ds(pl.multiple_of(256 * far, 256), 256)
            pbuf[k, rows, :] = pbuf[k, rows, :] + xhalf[across_first.index(k)]
        for h in halves[k]:
            for way in range(2):
                send_sum(k, h, way, 0)

    def st_sum(k, t):
        for h in halves[k]:
            came(rbuf.at[k, h, pl.ds(2 * t, 2 if t < 3 else 1)], rs_recv.at[flows.index((k, h)), t])
            for way in range(2):
                if t < steps(k, h, way) - 1:
                    rows = block_rows(k, h, sent_block(k, h, way, t + 1))
                    pbuf[k, rows, :] = pbuf[k, rows, :] + rbuf[k, h, slot(t, way)]
                    send_sum(k, h, way, t + 1)
        if t == 3:
            for h in halves[k]:
                total = pbuf[k, block_rows(k, h, z), :]
                for way in range(2):
                    total = total + rbuf[k, h, slot(steps(k, h, way) - 1, way)]
                sbuf[k, h] = total
            if k not in across_first:
                start(remote(sbuf.at[k, 1 - far], xrec.at[k], xs_send.at[0], xs_recv.at[k], (p, across)))

    core = p & 1
    side = (p >> 1) & 1
    mine = p & 3

    def spread_copy(t):
        return remote(e1s.at[t >> 2], e1r.at[p], e1_send.at[0], e1_recv.at[0], (t, q))

    def st_spread(k):
        def one(i, carry):
            spread_copy((p + i) & 15).start()
            return carry

        lax.fori_loop(1, GRID, one, 0)
        e1r[p] = e1s[p >> 2]

    y_rows = pl.ds(pl.multiple_of(ROWS * p, ROWS), ROWS)

    def y_copy(k, row):
        return remote(ystage.at[k], yq.at[k // 4, y_rows, :], yg_send.at[0], yg_recv.at[k // 4], (row, q))

    def st_panel(k):
        if k in across_first:
            total = sbuf[k, 0]
        else:
            came(xrec.at[k], xs_recv.at[k])
            total = sbuf[k, far] + xrec[k]
        y = total * (-mask_of(k, p))
        ystage[k] = y
        y_out[pl.ds(k, ROWS, stride=12), :] = y
        for up in (8, 4, 12, 0):
            row = 4 * (((p + up) & 15) >> 2) + k % 4
            if up:
                y_copy(k, row).start()
            else:

                @pl.when(mine != k % 4)
                def _():
                    y_copy(k, row).start()

                @pl.when(mine == k % 4)
                def _():
                    yq[k // 4, y_rows, :] = y

    def st_spread_wait(k):
        came(e1r.at[pl.ds(0, GRID - 1)], e1_recv.at[0])
        for n in range(NSUP):
            l_high[n], l_low[n] = split(e1r[:, n].reshape(WIDTH, 128).T)

    same = mine == (q >> 2)

    def e2_copy(n, w, t):
        return remote(
            e2s.at[n, w, t], e2r.at[n, q], e2_send.at[0], e2_recv.at[n], (p - mine + w, 4 * mine + t)
        )

    def st_diagonal(n):
        came(yq.at[n, pl.ds(0, ROWS * (GRID - 1)), :], yg_recv.at[n])
        y_high, y_low = split(yq[n])
        total = dot(l_high[n], y_high) + dot(l_high[n], y_low) + dot(l_low[n], y_high)
        for w in range(4):

            def put(t, tile, w=w):
                e2s[n, w, t] = tile

            pack(total[32 * w : 32 * w + 32, :], put)
        for w in range(4):
            for t in range(4):

                @pl.when(jnp.logical_or(mine != w, 4 * mine + t != q))
                def _():
                    e2_copy(n, w, t).start()

        @pl.when(same)
        def _():
            e2r[n, q] = e2s[n, mine, q & 3]

    def st_result(n):
        @pl.when(same)
        def _():
            came(e2r.at[n, pl.ds(0, GRID - 1)], e2_recv.at[n])

        @pl.when(jnp.logical_not(same))
        def _():
            came(e2r.at[n], e2_recv.at[n])

        total = jnp.sum(e2r[n], axis=0)
        parts = [total] + [pltpu.roll(total, 128 - 32 * u, 1) for u in range(1, 4)]
        square = jnp.concatenate(parts, axis=0)
        d_out[n] = piv_in[n] - square[:, :ROWS]

    def st_drain(n):
        if n == 0:

            @pl.when(jnp.logical_not(keeps))
            def _():
                went(src, a_send.at[0])

            @pl.when(jnp.logical_not(stays))
            def _():
                went(taken, land_send.at[0])

            went(xbuf.at[:, pl.ds(0, 15 * ROWS), :], xg_send.at[0])
            went(e1r.at[pl.ds(0, GRID - 1)], e1_send.at[0])
            return
        went(xbuf.at[pl.ds(0, 5), pl.ds(0, 256), :], xs_send.at[0])
        went(rbuf.at[pl.ds(0, UNITS - len(across_first) // 2)], rs_send.at[0])
        went(yq.at[:, pl.ds(0, ROWS * (GRID - 1)), :], yg_send.at[0])

    stages = {
        "drain": st_drain,
        "take": st_take,
        "prepare": st_prepare,
        "own": st_own,
        "second": st_second,
        "forward": st_forward,
        "product": st_product,
        "launch": st_launch,
        "panel": st_panel,
        "spread": st_spread,
        "arrived": st_spread_wait,
        "diagonal": st_diagonal,
        "result": st_result,
    }
    for t in range(4):
        stages[f"sum{t}"] = lambda k, t=t: st_sum(k, t)
    for name, k in ORDER:
        with jax.named_scope(f"{name}_{k}"):
            stages[name](k)

    @pl.when(same)
    def _():
        went(e2r.at[:, pl.ds(0, GRID - 1)], e2_send.at[0])

    @pl.when(jnp.logical_not(same))
    def _():
        went(e2r, e2_send.at[0])


def body(ancestor_inverse, factor_panel, pivot_inverse, structure):
    hbm = pl.BlockSpec(memory_space=pltpu.HBM)
    dma = pltpu.SemaphoreType.DMA
    panel, diagonal = pl.pallas_call(
        kernel,
        out_shape=(
            pltpu.VMEM((ROWS * NSUP * 4, 128), F32),
            pltpu.VMEM(pivot_inverse.shape, F32),
        ),
        in_specs=[hbm] * 4,
        out_specs=(pl.BlockSpec(memory_space=pltpu.VMEM),)*2,
        scratch_shapes=[
            pltpu.VMEM((WIDTH, WIDTH), F32),
            pltpu.VMEM((ROWS * NSUP * 4, 128), F32),
            pltpu.VMEM((NSUP, ROWS, ROWS), F32),
            pltpu.SMEM((NSUP, GRID), jnp.int32),
            pltpu.VMEM((WIDTH, WIDTH), BF16),
            pltpu.VMEM((WIDTH, WIDTH), BF16),
            pltpu.VMEM((UNITS, ROWS, COLS), F32),
            pltpu.VMEM((UNITS, ROWS, COLS), F32),
            pltpu.VMEM((UNITS, WIDTH, COLS), F32),
            pltpu.VMEM((UNITS, WIDTH, COLS), F32),
            pltpu.VMEM((UNITS, 2, 7, ROWS, COLS), F32),
            pltpu.VMEM((UNITS, 2, ROWS, COLS), F32),
            pltpu.VMEM((UNITS, ROWS, COLS), F32),
            pltpu.VMEM((len(FIRST_ACROSS), 256, COLS), F32),
            pltpu.VMEM((UNITS, ROWS, COLS), F32),
            pltpu.VMEM((NSUP, WIDTH, 128), F32),
            pltpu.VMEM((NSUP, 128, WIDTH), BF16),
            pltpu.VMEM((NSUP, 128, WIDTH), BF16),
            pltpu.VMEM((4, NSUP, ROWS, 128), F32),
            pltpu.VMEM((GRID, NSUP, ROWS, 128), F32),
            pltpu.VMEM((NSUP, 4, 4, 8, 128), F32),
            pltpu.VMEM((NSUP, GRID, 8, 128), F32),
            dma((4,)),
            dma((1,)),
            dma((UNITS,)),
            dma((1,)),
            dma((1,)),
            dma((UNITS, 5)),
            dma((1,)),
            dma((2 * UNITS - len(FIRST_ACROSS), 4)),
            dma((1,)),
            dma((UNITS,)),
            dma((1,)),
            dma((NSUP,)),
            dma((1,)),
            dma((1,)),
            dma((1,)),
            dma((NSUP,)),
        ],
        compiler_params=pltpu.CompilerParams(
            collective_id=0, has_side_effects=True, vmem_limit_bytes=VMEM_LIMIT
        ),
        name="level",
    )(
        pltpu.with_memory_space_constraint(ancestor_inverse.reshape(WIDTH, WIDTH), pltpu.HBM),
        pltpu.with_memory_space_constraint(factor_panel.reshape(ROWS * NSUP * 4, 128), pltpu.HBM),
        pltpu.with_memory_space_constraint(pivot_inverse, pltpu.HBM),
        pltpu.with_memory_space_constraint(structure.T, pltpu.HBM),
    )
    return panel.reshape(ROWS, 1, NSUP, WIDTH), diagonal


def solution(mesh):
    return jax.shard_map(
        body,
        mesh=mesh,
        in_specs=(
            P("prow", "pcol", None, None),
            P("pcol", "prow", None, None),
            P(None, "prow", "pcol"),
            P(),
        ),
        out_specs=(P("pcol", "prow", None, None), P(None, "prow", "pcol")),
        check_vma=False,
    )
```
